128 devices in a mesh: fc: 16 (over z, y_lo, core), tok: 8 (over x, y_hi).
Axes of the slice: x: 4, y: 4 (y_hi: 2, y_lo: 2; y = y_hi * 2 + y_lo), z: 4, core: 2. Of those that a mesh axis runs over, the one named last changes fastest.
Arguments:
- tokens: bfloat16 [16, 64, 128, 1024], P('fc', 'tok'), may hold values from -6 to 6
- slot_keys: bfloat16 [1024, 1024], replicated, may hold values from -2 to 2
- norm_gain: float32 [1024], replicated, may hold values from 0.25 to 1.75
- slot_gain: float32 [1024], replicated, may hold values from 0.25 to 1.75
- w_in: bfloat16 [256, 1024, 512], P(('fc', 'tok')), may hold values from -0.1875 to 0.1875
- w_out: bfloat16 [256, 512, 1024], P(('fc', 'tok')), may hold values from -0.25 to 0.25
- conv_weight: float32 [7, 7, 1024], replicated, may hold values from -0.875 to 0.875
- ln_gain: float32 [1024], replicated, may hold values from 0.25 to 1.75
- proj: bfloat16 [1024, 1024], replicated, may hold values from -0.1875 to 0.1875
- layer_scale: float32 [1024], replicated, may hold values from 0.25 to 1.75
Outputs:
- fields: bfloat16 [16, 64, 128, 1024], P('fc', 'tok')
The draws below stay inside these ranges and needn't reach their ends.
All inputs are finite; a program needn't handle non-finite values.
Results may differ from the reference program's by a relative error of at most 0.008.
The reference program's roundings to bfloat16 on the way (of `normed`, `dispatch`, `slot_in`, `hidden`, `slot_out`, `combine`, `state` and `normal`) count: a program that leaves them out, or rounds other values in their place, can miss the bound.
Values may be sent and summed in bfloat16 or wider, within the bound.
A program may use at most 64 MiB of HBM per device.

```python
import jax
import jax.numpy as jnp
from jax import lax

D = 1024
FF = 512
SLOTS_EXP = 4
KSIZE = 7
COLS = 128
MEMBERS = 16
ROWS = 64
EXPERTS = 256
SLOTS = 1024


def draw_slot_keys(key, part):
    base = jax.random.truncated_normal(jax.random.fold_in(key, 1), -6.0, 6.0, (D, SLOTS), jnp.float32) * D ** (-0.5)
    return base.astype(jnp.bfloat16)


def draw_tokens(key, part):
    base = jax.random.truncated_normal(jax.random.fold_in(key, 5), -6.0, 6.0, (MEMBERS, ROWS, COLS, D), jnp.float32)
    return base.astype(jnp.bfloat16)


def block_levels(key, extent, cuts, smallest, largest):
    def one(axis_at, blocks):
        steps = jax.random.uniform(jax.random.fold_in(jax.random.fold_in(key, 6), axis_at), (blocks,), jnp.float32, smallest / len(cuts), largest / len(cuts))
        return jnp.repeat(jnp.exp(steps), extent[axis_at] // blocks).reshape((-1,) + (1,) * (len(extent) - axis_at - 1))

    level = one(*cuts[0])
    for cut in cuts[1:]:
        level = level * one(*cut)
    return level


def gaussian(rng, dims, scale, reach, cuts=(), dtype=jnp.bfloat16):
    level = block_levels(rng, dims, cuts, -0.22, 0.18) if cuts else 1.0
    drawn = jax.random.normal(rng, dims, jnp.float32) * scale * level
    return jnp.minimum(jnp.maximum(drawn, -reach), reach).astype(dtype)


def setup_inputs(seed: int = 0) -> dict:
    keys = jax.random.split(jax.random.key(seed), 11)
    tokens = draw_tokens(jax.random.fold_in(keys[10], 71), 0)
    slot_keys = draw_slot_keys(jax.random.fold_in(keys[10], 71), 0)
    norm_gain = jnp.clip(1.0 + 0.15 * jax.random.normal(keys[2], (D,), jnp.float32), 0.25, 1.75)
    slot_gain = jnp.clip(1.0 + 0.15 * jax.random.normal(keys[3], (D,), jnp.float32), 0.25, 1.75)
    w_in = gaussian(keys[4], (EXPERTS, D, FF), D ** -0.5, 0.1875, ((0, 128),))
    w_out = gaussian(keys[5], (EXPERTS, FF, D), FF ** -0.5, 0.25, ((0, 128),))
    conv_weight = gaussian(keys[6], (KSIZE, KSIZE, D), (KSIZE * KSIZE) ** -0.5, 0.875, (), jnp.float32)
    ln_gain = jnp.clip(1.0 + 0.15 * jax.random.normal(keys[7], (D,), jnp.float32), 0.25, 1.75)
    proj = gaussian(keys[8], (D, D), D ** -0.5, 0.1875)
    layer_scale = jnp.clip(1.0 + 0.15 * jax.random.normal(keys[9], (D,), jnp.float32), 0.25, 1.75)
    return {"tokens": tokens, "slot_keys": slot_keys, "norm_gain": norm_gain, "slot_gain": slot_gain, "w_in": w_in, "w_out": w_out, "conv_weight": conv_weight, "ln_gain": ln_gain, "proj": proj, "layer_scale": layer_scale}


def rms_scale(value, gain):
    return value * lax.rsqrt(lax.optimization_barrier(jnp.mean(value * value, axis=-1, keepdims=True)) + 1e-06) * gain

def reference(tokens, slot_keys, norm_gain, slot_gain, w_in, w_out, conv_weight, ln_gain, proj, layer_scale):
    members = tokens.shape[0]
    flat = tokens.reshape(members, ROWS * COLS, D)

    def dispatch_one(cells):
        normed = rms_scale(cells.astype(jnp.float32), norm_gain).astype(jnp.bfloat16)
        logits = jnp.dot(normed, slot_keys, preferred_element_type=jnp.float32)
        peak = lax.optimization_barrier(jnp.max(logits, axis=0))
        shifted = jnp.exp(logits - peak)
        dispatch = shifted.astype(jnp.bfloat16)
        numer = jnp.dot(dispatch.T, cells, preferred_element_type=jnp.float32)
        slot_in = rms_scale(numer, slot_gain).astype(jnp.bfloat16)
        return (slot_in, logits)
    slot_in, logits = lax.map(dispatch_one, flat)
    grouped = slot_in.reshape(members, EXPERTS, SLOTS_EXP, D).astype(jnp.float32)
    hidden = jax.nn.gelu(jnp.einsum('mesd,edf->mesf', grouped, w_in.astype(jnp.float32))).astype(jnp.bfloat16)
    slot_out = jnp.einsum('mesf,efd->mesd', hidden.astype(jnp.float32), w_out.astype(jnp.float32)).astype(jnp.bfloat16)
    slot_out = slot_out.reshape(members, SLOTS, D)

    def block_one(packed):
        cells, member_logits, outputs = packed
        combine = jax.nn.softmax(member_logits, axis=-1).astype(jnp.bfloat16)
        mixed = jnp.dot(combine, outputs, preferred_element_type=jnp.float32)
        state = (cells.astype(jnp.float32) + mixed).astype(jnp.bfloat16).reshape(ROWS, COLS, D)
        padded = jnp.pad(state, ((3, 3), (0, 0), (0, 0)))
        padded = jnp.concatenate([padded[:, COLS - 3:], padded, padded[:, :3]], axis=1)
        conv = jnp.zeros((ROWS, COLS, D), jnp.float32)
        for row_tap in range(KSIZE):
            for col_tap in range(KSIZE):
                conv = conv + padded[row_tap:row_tap + ROWS, col_tap:col_tap + COLS].astype(jnp.float32) * conv_weight[row_tap, col_tap]
        center = conv - lax.optimization_barrier(jnp.mean(conv, axis=-1, keepdims=True))
        spread = lax.optimization_barrier(jnp.mean(center * center, axis=-1, keepdims=True))
        normal = (center * lax.rsqrt(spread + 1e-06) * ln_gain).astype(jnp.bfloat16)
        branch = jnp.dot(normal.reshape(ROWS * COLS, D), proj, preferred_element_type=jnp.float32)
        result = state.reshape(ROWS * COLS, D).astype(jnp.float32) + layer_scale * jax.nn.gelu(branch)
        return result.astype(jnp.bfloat16).reshape(ROWS, COLS, D)
    return lax.map(block_one, (flat, logits, slot_out))
```

```python
import jax
import jax.numpy as jnp
from jax import lax
from jax.experimental import pallas as pl
from jax.experimental.pallas import tpu as pltpu
from jax.sharding import Mesh
from jax.sharding import PartitionSpec as P

BF = jnp.bfloat16
F32 = jnp.float32
TOK = ("tok_0", "tok_1")
FC_TOK = ("fc", "tok_0", "tok_1")


def tree_sum(terms):
    terms = list(terms)
    while len(terms) > 1:
        nxt = [terms[i] + terms[i + 1] for i in range(0, len(terms) - 1, 2)]
        if len(terms) % 2:
            nxt.append(terms[-1])
        terms = nxt
    return terms[0]


def block_kernel(
    state_ref, cw_ref, gain_ref, scale_ref, proj_hbm, out_hbm,
    wide, taps, conv, outs, proj, proj_sem, out_sem,
):
    width = state_ref.shape[2]
    chunks = width // 128
    load_proj = pltpu.make_async_copy(proj_hbm, proj, proj_sem)
    load_proj.start()

    @pl.loop(0, chunks)
    def _(k):
        lane = pl.ds(pl.multiple_of(k * 128, 128), 128)
        for tap in range(49):
            row = cw_ref[pl.ds(tap, 1), lane]
            taps[tap] = jnp.broadcast_to(row, (16, 128)).astype(BF)

        @pl.loop(0, 14)
        def _(r):
            v = state_ref[r, :, lane].astype(F32)
            wide[r, pl.ds(8, 128), :] = v
            wide[r, pl.ds(0, 8), :] = v[120:128]
            wide[r, pl.ds(136, 8), :] = v[0:8]

        @pl.loop(0, 8)
        def _(i):
            acc = [[None] * 4, [None] * 4]
            for b in range(7):
                wv = [taps[a * 7 + b] for a in range(7)]
                for blk in range(2):
                    start = i * 16 + (8 * blk + 5 + b)
                    v = [wide[r, pl.ds(start, 8), :] for r in range(14)]
                    pk = [jnp.concatenate([v[q], v[q + 4]], axis=0).astype(BF) for q in range(10)]
                    for p in range(4):
                        t = tree_sum(pk[p + a] * wv[a] for a in range(7))
                        acc[blk][p] = t if acc[blk][p] is None else acc[blk][p] + t
            for blk in range(2):
                for p in range(4):
                    f = acc[blk][p].astype(F32)
                    at = pl.multiple_of(i * 16 + 8 * blk, 8)
                    conv[p, pl.ds(at, 8), lane] = f[0:8]
                    conv[p + 4, pl.ds(at, 8), lane] = f[8:16]

    load_proj.wait()

    @pl.loop(0, 8)
    def _(r):
        c = conv[r]
        mean = jnp.mean(c, axis=-1, keepdims=True)
        center = c - mean
        spread = jnp.mean(center * center, axis=-1, keepdims=True)
        normal = (center * lax.rsqrt(spread + 1e-06) * gain_ref[...]).astype(BF)
        branch = jnp.dot(normal, proj[...], preferred_element_type=F32)
        res = state_ref[r + 3].astype(F32) + scale_ref[...] * jax.nn.gelu(branch)
        outs[r] = res.astype(BF)
        pltpu.make_async_copy(outs.at[r], out_hbm.at[r], out_sem.at[r]).start()

    for r in range(8):
        pltpu.make_async_copy(outs.at[r], out_hbm.at[r], out_sem.at[r]).wait()


def block(state14, conv_weight, ln_gain, layer_scale, proj):
    width = state14.shape[2]
    vm = pl.BlockSpec(memory_space=pltpu.VMEM)
    anyspec = pl.BlockSpec(memory_space=pl.ANY)
    return pl.pallas_call(
        block_kernel,
        out_shape=jax.ShapeDtypeStruct((8, 128, width), BF),
        in_specs=[vm, vm, vm, vm, anyspec],
        out_specs=anyspec,
        scratch_shapes=[
            pltpu.VMEM((14, 144, 128), F32),
            pltpu.VMEM((49, 16, 128), BF),
            pltpu.VMEM((8, 128, width), F32),
            pltpu.VMEM((8, 128, width), BF),
            pltpu.VMEM((width, width), BF),
            pltpu.SemaphoreType.DMA,
            pltpu.SemaphoreType.DMA((8,)),
        ],
        compiler_params=pltpu.CompilerParams(vmem_limit_bytes=60 * 1024 * 1024),
        name="block",
    )(state14, conv_weight.reshape(49, width), ln_gain.reshape(1, width), layer_scale.reshape(1, width), proj)


def from_everyone(x, axis):
    size = lax.axis_size(axis)
    return lax.all_to_all(jnp.broadcast_to(x[None], (size, *x.shape)), axis, 0, 0, tiled=True)


def of_everyone(x, axis):
    return from_everyone(x, axis).max(axis=0)


def summed_rows(x, axes, dim):
    for axis in axes:
        x = lax.psum_scatter(x, axis, scatter_dimension=dim, tiled=True)
    return x


def joined_along(pieces, dim):
    pieces = jnp.moveaxis(pieces, 0, dim)
    dims = pieces.shape
    return pieces.reshape(*dims[:dim], dims[dim] * dims[dim + 1], *dims[dim + 2 :])


def gathered_copies(x, axis, dim):
    return joined_along(from_everyone(x, axis), dim)


def with_halo(block, sides, width):
    for axis, dim in sides:
        count = lax.axis_size(axis)
        forward = [(i, i + 1) for i in range(count - 1)]
        backward = [(target, source) for source, target in forward]
        low = lax.ppermute(
            lax.slice_in_dim(block, block.shape[dim] - width, None, axis=dim), axis, forward
        )
        high = lax.ppermute(lax.slice_in_dim(block, 0, width, axis=dim), axis, backward)
        block = jnp.concatenate([low, block, high], axis=dim)
    return block


def rms_scale(value, gain):
    return value * lax.rsqrt(jnp.mean(value * value, axis=-1, keepdims=True) + 1e-06) * gain


def local(
    tokens, slot_keys, norm_gain, slot_gain, w_in, w_out, conv_weight, ln_gain, proj, layer_scale
):
    rows = tokens.shape[1]
    cols = tokens.shape[2]
    width = tokens.shape[3]
    count_fc = lax.axis_size("fc")
    count_tok = lax.axis_size(TOK)
    slot_total = slot_keys.shape[1]
    slot_dev = slot_total // (count_fc * count_tok)
    cells = tokens.reshape(rows * cols, width)
    normed = rms_scale(cells.astype(jnp.float32), norm_gain).astype(jnp.bfloat16)
    logits = jnp.dot(normed, slot_keys, preferred_element_type=jnp.float32)
    peak = of_everyone(jnp.max(logits, axis=0), TOK)
    shifted = jnp.exp(logits - peak)
    dispatch = shifted.astype(jnp.bfloat16)
    numer = lax.dot_general(
        dispatch, cells, (((0,), (0,)), ((), ())), preferred_element_type=jnp.float32
    )
    numer = numer.reshape(count_fc, count_tok * slot_dev, width)
    numer = summed_rows(numer.astype(jnp.bfloat16), TOK, 1).astype(jnp.float32)
    local_in = rms_scale(numer, slot_gain).astype(jnp.bfloat16)
    slot_in = lax.all_to_all(local_in, "fc", split_axis=0, concat_axis=0, tiled=True)
    grouped = slot_in.reshape(count_fc, w_in.shape[0], slot_dev // w_in.shape[0], width)
    hidden = jax.nn.gelu(
        jnp.einsum("mesd,edf->mesf", grouped, w_in, preferred_element_type=jnp.float32)
    ).astype(jnp.bfloat16)
    expert_out = jnp.einsum(
        "mesf,efd->mesd", hidden, w_out, preferred_element_type=jnp.float32
    ).astype(jnp.bfloat16)
    expert_out = expert_out.reshape(count_fc, slot_dev, width)
    returned = lax.all_to_all(expert_out, "fc", split_axis=0, concat_axis=0, tiled=True)
    every_slot = gathered_copies(returned, TOK, 1).reshape(slot_total, width)
    combine = jax.nn.softmax(logits, axis=-1).astype(jnp.bfloat16)
    mixed = jnp.dot(combine, every_slot, preferred_element_type=jnp.float32)
    state = (cells.astype(jnp.float32) + mixed).astype(jnp.bfloat16).reshape(rows, cols, width)
    padded = with_halo(state, ((TOK, 0),), 3)
    result = block(padded, conv_weight, ln_gain, layer_scale, proj)
    return result.reshape(1, rows, cols, width)


def solution(mesh):
    finer = Mesh(mesh.devices.reshape(mesh.shape["fc"], 4, 2), ("fc", "tok_0", "tok_1"))
    in_specs = (
        P("fc", TOK, None, None),
        P(),
        P(),
        P(),
        P(FC_TOK, None, None),
        P(FC_TOK, None, None),
        P(),
        P(),
        P(),
        P(),
    )
    out_specs = P("fc", TOK, None, None)
    return jax.shard_map(local, mesh=finer, in_specs=in_specs, out_specs=out_specs, check_vma=False)
```

```python
import jax
import jax.numpy as jnp
from jax import lax
from jax.experimental import pallas as pl
from jax.experimental.pallas import tpu as pltpu
from jax.sharding import PartitionSpec as P

BF = jnp.bfloat16
F32 = jnp.float32
MESH = pl.DeviceIdType.MESH
MEMBERS_AX = 16
NCH = 4


def rms_scale(value, gain):
    return value * lax.rsqrt(jnp.mean(value * value, axis=-1, keepdims=True) + 1e-06) * gain


def fold_halves(v):
    half = v.shape[-1] // 2
    return jnp.concatenate([v[..., :half], v[..., half:]], axis=-2)


def unfold_halves(v):
    rows = v.shape[-2] // 2
    return jnp.concatenate([v[..., :rows, :], v[..., rows:, :]], axis=-1)


def mix_kernel(
    tok_hbm, keys_hbm, ngain_ref, sgain_ref, win_hbm, wout_hbm, state_hbm,
    cells, keys, win, wout, logits, combine, disp, numer, rx, ysend, yrecv, keep,
    asend, arecv, bsend, brecv, part, every, state, peaks, load_sem,
    peak_ss, peak_rs, halo_ss, halo_rs, x_ss, x_rs, y_ss, y_rs, a_ss, a_rs, b_ss, b_rs,
    p_ss, p_rs, g_ss, g_rs, out_sem,
):
    nf, nt = MEMBERS_AX, 8
    width = cells.shape[2]
    cw = width // NCH
    f = lax.axis_index("fc")
    t = lax.axis_index("tok")
    x = lax.div(t, 2)
    h = lax.rem(t, 2)

    loads = [
        pltpu.make_async_copy(tok_hbm, cells.at[pl.ds(3, 8)], load_sem.at[0]),
        pltpu.make_async_copy(keys_hbm, keys, load_sem.at[1]),
        pltpu.make_async_copy(win_hbm, win, load_sem.at[2]),
        pltpu.make_async_copy(wout_hbm, wout, load_sem.at[3]),
    ]
    for c in loads:
        c.start()

    def at_tok(k):
        return {"fc": f, "tok": k}

    def at_fc(k):
        return {"fc": k, "tok": t}

    barrier = pltpu.get_barrier_semaphore()
    for d in range(1, nt):
        pl.semaphore_signal(barrier, inc=1, device_id=at_tok(lax.rem(t + d, nt)), device_id_type=MESH)
    for d in range(1, nf):
        pl.semaphore_signal(barrier, inc=1, device_id=at_fc(lax.rem(f + d, nf)), device_id_type=MESH)

    def remote(src, dst, ss, rs, dev):
        return pltpu.make_async_remote_copy(
            src_ref=src, dst_ref=dst, send_sem=ss, recv_sem=rs, device_id=dev, device_id_type=MESH
        )

    loads[0].wait()
    loads[1].wait()

    def logits_of(v):
        normed = rms_scale(v.astype(F32), ngain_ref[...]).astype(BF)
        return jnp.dot(normed, keys[...], preferred_element_type=F32)

    def softmax_of(l):
        e = jnp.exp(l - jnp.max(l, axis=-1, keepdims=True))
        return (e / jnp.sum(e, axis=-1, keepdims=True)).astype(BF)

    def first(r, peak):
        v = cells[pl.ds(3 + 2 * r, 2)].reshape(256, width)
        l = logits_of(v)
        logits[pl.ds(2 * r, 2)] = l.reshape(2, 128, width)
        return jnp.maximum(peak, jnp.max(l.reshape(32, 8, width), axis=0))

    peak = lax.fori_loop(0, 4, first, jnp.full((8, width), -jnp.inf, F32))
    peaks[t] = jnp.max(peak, axis=0, keepdims=True)

    pl.semaphore_wait(barrier, nt + nf - 2)
    peak_copies = []
    for d in range(1, nt):
        k = lax.rem(t + d, nt)
        c = remote(peaks.at[t], peaks.at[t], peak_ss.at[d - 1], peak_rs.at[d - 1], at_tok(k))
        c.start()
        peak_copies.append(c)

    def halo_copies(part_at):
        low = remote(
            cells.at[8 + part_at], cells.at[part_at], halo_ss.at[0, part_at], halo_rs.at[0, part_at], at_tok(t + 1)
        )
        high = remote(
            cells.at[3 + part_at], cells.at[11 + part_at], halo_ss.at[1, part_at], halo_rs.at[1, part_at], at_tok(t - 1)
        )
        return low, high

    def start_halo(part_at):
        low, high = halo_copies(part_at)

        @pl.when(t < nt - 1)
        def _():
            low.start()

        @pl.when(t > 0)
        def _():
            high.start()

    start_halo(0)

    @pl.when(t == 0)
    def _():
        cells[pl.ds(0, 3)] = jnp.zeros((3, 128, width), BF)

    @pl.when(t == nt - 1)
    def _():
        cells[pl.ds(11, 3)] = jnp.zeros((3, 128, width), BF)

    @pl.loop(0, 8)
    def _(r):
        combine[3 + r] = softmax_of(logits[r])

    for c in peak_copies:
        c.wait_recv()
    top = peaks[0]
    for k in range(1, nt):
        top = jnp.maximum(top, peaks[k])

    @pl.loop(0, 8)
    def _(r):
        shifted = jnp.exp(logits[r] - top)
        disp[:, pl.ds(pl.multiple_of(r * 128, 128), 128)] = shifted.T.astype(BF)

    x_copies = []
    for n in range(NCH):
        lane = pl.ds(n * cw, cw)
        own = cells[pl.ds(3, 8), :, lane].reshape(1024, cw)
        numer[:, :, :, lane] = (
            jnp.dot(disp[...], own, preferred_element_type=F32).astype(BF).reshape(nf, 4, 16, cw)
        )
        row = []
        for d in range(1, 4):
            k = lax.rem(x + d, 4)
            c = remote(
                numer.at[:, k, :, lane], rx.at[d - 1, :, :, lane], x_ss.at[n, d - 1], x_rs.at[n, d - 1],
                at_tok(k * 2 + h),
            )
            c.start()
            row.append(c)
        x_copies.append(row)

    y_copies = []
    for n in range(NCH):
        lane = pl.ds(n * cw, cw)
        for c in x_copies[n]:
            c.wait_recv()
        total = numer[:, x, :, lane].astype(F32)
        for d in range(3):
            total = total + rx[d, :, :, lane].astype(F32)
        low = total[:, 0:8].reshape(nf * 8, cw)
        high = total[:, 8:16].reshape(nf * 8, cw)
        ysend[:, lane] = jnp.where(h == 0, high, low).astype(BF)
        keep[:, lane] = jnp.where(h == 0, low, high)
        c = remote(
            ysend.at[:, lane], yrecv.at[:, lane], y_ss.at[n], y_rs.at[n], at_tok(x * 2 + 1 - h)
        )
        c.start()
        y_copies.append(c)
        if n == 1:
            start_halo(1)

    for c in y_copies:
        c.wait_recv()
    local_in = rms_scale(keep[...] + yrecv[...].astype(F32), sgain_ref[...])
    asend[...] = fold_halves(local_in.reshape(nf, 8, width)).astype(BF)
    arecv[f] = asend[f]
    a_copies = []
    for d in range(1, nf):
        k = lax.rem(f + d, nf)
        c = remote(asend.at[k], arecv.at[f], a_ss.at[d - 1], a_rs.at[d - 1], at_fc(k))
        c.start()
        a_copies.append(c)
    loads[2].wait()
    loads[3].wait()
    for c in a_copies:
        c.wait_recv()

    lhs = unfold_halves(arecv[...].astype(F32)).reshape(nf * 8, width).astype(BF)
    which = lax.rem(lax.broadcasted_iota(jnp.int32, (nf * 8, 1), 0), 8) < 4
    hid = jnp.where(
        which,
        jnp.dot(lhs, win[0], preferred_element_type=F32),
        jnp.dot(lhs, win[1], preferred_element_type=F32),
    )
    hid = jax.nn.gelu(hid).astype(BF)
    out = jnp.where(
        which,
        jnp.dot(hid, wout[0], preferred_element_type=F32),
        jnp.dot(hid, wout[1], preferred_element_type=F32),
    )
    bsend[...] = fold_halves(out.reshape(nf, 8, width)).astype(BF)
    brecv[f] = bsend[f]
    b_copies = []
    for d in range(1, nf):
        k = lax.rem(f + d, nf)
        c = remote(bsend.at[k], brecv.at[f], b_ss.at[d - 1], b_rs.at[d - 1], at_fc(k))
        c.start()
        b_copies.append(c)
    for c in b_copies:
        c.wait_recv()

    pair = remote(brecv, part, p_ss, p_rs, at_tok(x * 2 + 1 - h))
    pair.start()
    start_halo(2)
    pair.wait_recv()
    mine = unfold_halves(brecv[...].astype(F32))
    theirs = unfold_halves(part[...].astype(F32))
    low = jnp.where(h == 0, mine, theirs)
    high = jnp.where(h == 0, theirs, mine)
    every[:, x] = jnp.concatenate([low, high], axis=1).astype(BF)

    g_copies = []
    for n in range(NCH):
        lane = pl.ds(n * cw, cw)
        row = []
        for d in range(1, 4):
            k = lax.rem(x + d, 4)
            c = remote(
                every.at[:, x, :, lane], every.at[:, x, :, lane], g_ss.at[n, d - 1], g_rs.at[n, d - 1],
                at_tok(k * 2 + h),
            )
            c.start()
            row.append(c)
        g_copies.append(row)

    for p in range(3):
        lo_copy, hi_copy = halo_copies(p)

        @pl.when(t > 0)
        def _():
            lo_copy.wait_recv()

        @pl.when(t < nt - 1)
        def _():
            hi_copy.wait_recv()

    @pl.loop(0, 6)
    def _(i):
        r = i + 8 * lax.div(i, 3)
        combine[r] = softmax_of(logits_of(cells[r]))

    outs = []
    rows = 7 * 128
    for n in range(NCH):
        lane = pl.ds(n * cw, cw)
        for c in g_copies[n]:
            c.wait_recv()
        rhs = every[:, :, :, lane].reshape(1024, cw)

        @pl.loop(0, 2)
        def _(b):
            mixed = jnp.dot(
                combine[pl.ds(b * 7, 7)].reshape(rows, width), rhs, preferred_element_type=F32
            )
            v = cells[pl.ds(b * 7, 7), :, lane].reshape(rows, cw).astype(F32) + mixed
            at = lax.broadcasted_iota(jnp.int32, (rows, 1), 0) + (b * rows + (8 * t - 3) * 128)
            inside = jnp.logical_and(at >= 0, at < 64 * 128)
            v = jnp.where(inside, v, 0.0)
            state[pl.ds(b * 7, 7), :, lane] = v.astype(BF).reshape(7, 128, cw)

        o = pltpu.make_async_copy(state.at[:, :, lane], state_hbm.at[:, :, lane], out_sem.at[n])
        o.start()
        outs.append(o)

    for c in peak_copies + [c for row in x_copies for c in row] + y_copies + a_copies + b_copies:
        c.wait_send()
    pair.wait_send()
    for row in g_copies:
        for c in row:
            c.wait_send()
    for p in range(3):
        lo_copy, hi_copy = halo_copies(p)

        @pl.when(t < nt - 1)
        def _():
            lo_copy.wait_send()

        @pl.when(t > 0)
        def _():
            hi_copy.wait_send()

    for o in outs:
        o.wait()


def mixed_state(tokens, slot_keys, norm_gain, slot_gain, w_in, w_out):
    width = tokens.shape[2]
    vm = pl.BlockSpec(memory_space=pltpu.VMEM)
    anyspec = pl.BlockSpec(memory_space=pl.ANY)
    dma = pltpu.SemaphoreType.DMA
    nf = MEMBERS_AX
    return pl.pallas_call(
        mix_kernel,
        out_shape=jax.ShapeDtypeStruct((14, 128, width), BF),
        in_specs=[anyspec, anyspec, vm, vm, anyspec, anyspec],
        out_specs=anyspec,
        scratch_shapes=[
            pltpu.VMEM((14, 128, width), BF),
            pltpu.VMEM((width, width), BF),
            pltpu.VMEM(w_in.shape, BF),
            pltpu.VMEM(w_out.shape, BF),
            pltpu.VMEM((8, 128, width), F32),
            pltpu.VMEM((14, 128, width), BF),
            pltpu.VMEM((width, 1024), BF),
            pltpu.VMEM((nf, 4, 16, width), BF),
            pltpu.VMEM((3, nf, 16, width), BF),
            pltpu.VMEM((nf * 8, width), BF),
            pltpu.VMEM((nf * 8, width), BF),
            pltpu.VMEM((nf * 8, width), F32),
            pltpu.VMEM((nf, 16, width // 2), BF),
            pltpu.VMEM((nf, 16, width // 2), BF),
            pltpu.VMEM((nf, 16, width // 2), BF),
            pltpu.VMEM((nf, 16, width // 2), BF),
            pltpu.VMEM((nf, 16, width // 2), BF),
            pltpu.VMEM((nf, 4, 16, width), BF),
            pltpu.VMEM((14, 128, width), BF),
            pltpu.VMEM((8, 1, width), F32),
            dma((4,)),
            dma((7,)), dma((7,)),
            dma((2, 3)), dma((2, 3)),
            dma((NCH, 3)), dma((NCH, 3)),
            dma((NCH,)), dma((NCH,)),
            dma((15,)), dma((15,)),
            dma((15,)), dma((15,)),
            dma, dma,
            dma((NCH, 3)), dma((NCH, 3)),
            dma((NCH,)),
        ],
        compiler_params=pltpu.CompilerParams(
            collective_id=0, has_side_effects=True, vmem_limit_bytes=62 * 1024 * 1024
        ),
        name="mix",
    )(tokens, slot_keys, norm_gain.reshape(1, width), slot_gain.reshape(1, width), w_in, w_out)


def tree_sum(terms):
    terms = list(terms)
    while len(terms) > 1:
        nxt = [terms[i] + terms[i + 1] for i in range(0, len(terms) - 1, 2)]
        if len(terms) % 2:
            nxt.append(terms[-1])
        terms = nxt
    return terms[0]


def block_kernel(
    state_ref, cw_ref, gain_ref, scale_ref, proj_hbm, out_hbm,
    wide, taps, conv, outs, proj, proj_sem, out_sem,
):
    width = state_ref.shape[2]
    chunks = width // 128
    load_proj = pltpu.make_async_copy(proj_hbm, proj, proj_sem)
    load_proj.start()

    @pl.loop(0, chunks)
    def _(k):
        lane = pl.ds(pl.multiple_of(k * 128, 128), 128)
        for tap in range(49):
            row = cw_ref[pl.ds(tap, 1), lane]
            taps[tap] = jnp.broadcast_to(row, (16, 128)).astype(BF)

        @pl.loop(0, 14)
        def _(r):
            v = state_ref[r, :, lane].astype(F32)
            wide[r, pl.ds(8, 128), :] = v
            wide[r, pl.ds(0, 8), :] = v[120:128]
            wide[r, pl.ds(136, 8), :] = v[0:8]

        @pl.loop(0, 8)
        def _(i):
            acc = [[None] * 4, [None] * 4]
            for b in range(7):
                wv = [taps[a * 7 + b] for a in range(7)]
                for blk in range(2):
                    start = i * 16 + (8 * blk + 5 + b)
                    v = [wide[r, pl.ds(start, 8), :] for r in range(14)]
                    pk = [jnp.concatenate([v[q], v[q + 4]], axis=0).astype(BF) for q in range(10)]
                    for p in range(4):
                        t = tree_sum(pk[p + a] * wv[a] for a in range(7))
                        acc[blk][p] = t if acc[blk][p] is None else acc[blk][p] + t
            for blk in range(2):
                for p in range(4):
                    f = acc[blk][p].astype(F32)
                    at = pl.multiple_of(i * 16 + 8 * blk, 8)
                    conv[p, pl.ds(at, 8), lane] = f[0:8]
                    conv[p + 4, pl.ds(at, 8), lane] = f[8:16]

    load_proj.wait()

    @pl.loop(0, 8)
    def _(r):
        c = conv[r]
        mean = jnp.mean(c, axis=-1, keepdims=True)
        center = c - mean
        spread = jnp.mean(center * center, axis=-1, keepdims=True)
        normal = (center * lax.rsqrt(spread + 1e-06) * gain_ref[...]).astype(BF)
        branch = jnp.dot(normal, proj[...], preferred_element_type=F32)
        res = state_ref[r + 3].astype(F32) + scale_ref[...] * jax.nn.gelu(branch)
        outs[r] = res.astype(BF)
        pltpu.make_async_copy(outs.at[r], out_hbm.at[r], out_sem.at[r]).start()

    for r in range(8):
        pltpu.make_async_copy(outs.at[r], out_hbm.at[r], out_sem.at[r]).wait()


def block(state14, conv_weight, ln_gain, layer_scale, proj):
    width = state14.shape[2]
    vm = pl.BlockSpec(memory_space=pltpu.VMEM)
    anyspec = pl.BlockSpec(memory_space=pl.ANY)
    return pl.pallas_call(
        block_kernel,
        out_shape=jax.ShapeDtypeStruct((8, 128, width), BF),
        in_specs=[vm, vm, vm, vm, anyspec],
        out_specs=anyspec,
        scratch_shapes=[
            pltpu.VMEM((14, 144, 128), F32),
            pltpu.VMEM((49, 16, 128), BF),
            pltpu.VMEM((8, 128, width), F32),
            pltpu.VMEM((8, 128, width), BF),
            pltpu.VMEM((width, width), BF),
            pltpu.SemaphoreType.DMA,
            pltpu.SemaphoreType.DMA((8,)),
        ],
        compiler_params=pltpu.CompilerParams(vmem_limit_bytes=60 * 1024 * 1024),
        name="block",
    )(state14, conv_weight.reshape(49, width), ln_gain.reshape(1, width), layer_scale.reshape(1, width), proj)


def local(
    tokens, slot_keys, norm_gain, slot_gain, w_in, w_out, conv_weight, ln_gain, proj, layer_scale
):
    state = mixed_state(tokens[0], slot_keys, norm_gain, slot_gain, w_in, w_out)
    return block(state, conv_weight, ln_gain, layer_scale, proj)[None]


def solution(mesh):
    in_specs = (
        P("fc", "tok", None, None),
        P(),
        P(),
        P(),
        P(("fc", "tok"), None, None),
        P(("fc", "tok"), None, None),
        P(),
        P(),
        P(),
        P(),
    )
    out_specs = P("fc", "tok", None, None)
    return jax.shard_map(local, mesh=mesh, in_specs=in_specs, out_specs=out_specs, check_vma=False)
```

```python
import jax
import jax.numpy as jnp
from jax import lax
from jax.experimental import pallas as pl
from jax.experimental.pallas import tpu as pltpu
from jax.sharding import PartitionSpec as P

BF = jnp.bfloat16
F32 = jnp.float32
MESH = pl.DeviceIdType.MESH
MEMBERS_AX = 16
NCH = 4
AT_SEND, AT_RETURN, LATE = (0,), (1,), (2,)


def rms_scale(value, gain):
    return value * lax.rsqrt(jnp.mean(value * value, axis=-1, keepdims=True) + 1e-06) * gain


def fold_halves(v):
    half = v.shape[-1] // 2
    return jnp.concatenate([v[..., :half], v[..., half:]], axis=-2)


def unfold_halves(v):
    rows = v.shape[-2] // 2
    return jnp.concatenate([v[..., :rows, :], v[..., rows:, :]], axis=-1)


def mix_kernel(
    tok_hbm, keys_hbm, ngain_ref, sgain_ref, win_hbm, wout_hbm, cw_ref, lgain_ref, scale_ref, proj_hbm,
    out_hbm,
    cells, keys, win, wout, logits, combine, disp, numer, passed, rx, ysend, yrecv, keep,
    asend, arecv, bsend, every, joined, state, wide, taps, conv, even, odd, outs, proj, peaks, tops, shrink, load_sem,
    peak_ss, peak_rs, top_ss, top_rs, halo_ss, halo_rs, w_ss, w_rs, x_ss, x_rs, y_ss, y_rs, a_ss, a_rs, b_ss, b_rs,
    p_ss, p_rs, g_ss, g_rs, o_ss, o_rs, out_sem,
):
    nf, nt = MEMBERS_AX, 8
    width = cells.shape[2]
    cw = width // NCH
    f = lax.axis_index("fc")
    t = lax.axis_index("tok")
    x = lax.div(t, 2)
    h = lax.rem(t, 2)

    def at_tok(k):
        return {"fc": f, "tok": k}

    def at_fc(k):
        return {"fc": k, "tok": t}

    right, left, across = lax.rem(x + 1, 4), lax.rem(x + 3, 4), lax.rem(x + 2, 4)
    to_right, to_left, to_pair = at_tok(right * 2 + h), at_tok(left * 2 + h), at_tok(x * 2 + 1 - h)

    loads = [
        pltpu.make_async_copy(tok_hbm, cells.at[pl.ds(3, 8)], load_sem.at[0]),
        pltpu.make_async_copy(keys_hbm, keys, load_sem.at[1]),
        pltpu.make_async_copy(win_hbm, win, load_sem.at[2]),
        pltpu.make_async_copy(wout_hbm, wout, load_sem.at[3]),
        pltpu.make_async_copy(proj_hbm, proj, load_sem.at[4]),
    ]
    loads[0].start()
    loads[1].start()

    barrier = pltpu.get_barrier_semaphore()
    for d in range(1, nt):
        pl.semaphore_signal(barrier, inc=1, device_id=at_tok(lax.rem(t + d, nt)), device_id_type=MESH)
    for d in range(1, nf):
        pl.semaphore_signal(barrier, inc=1, device_id=at_fc(lax.rem(f + d, nf)), device_id_type=MESH)

    def remote(src, dst, ss, rs, dev):
        return pltpu.make_async_remote_copy(
            src_ref=src, dst_ref=dst, send_sem=ss, recv_sem=rs, device_id=dev, device_id_type=MESH
        )

    loads[0].wait()
    pl.semaphore_wait(barrier, nt + nf - 2)

    def halo_low(p):
        return remote(
            cells.at[8 + p], cells.at[p], halo_ss.at[0, p], halo_rs.at[0, p], at_tok(t + 1)
        )

    def halo_high(p):
        return remote(
            cells.at[3 + p], cells.at[11 + p], halo_ss.at[1, p], halo_rs.at[1, p], at_tok(t - 1)
        )

    @pl.when(h == 0)
    def _():
        for p in range(3):
            halo_low(p).start()

    @pl.when(h == 1)
    def _():
        for p in range(3):
            halo_high(p).start()

    def start_cross(parts):
        @pl.when(jnp.logical_and(h == 1, t < nt - 1))
        def _():
            for p in parts:
                halo_low(p).start()

        @pl.when(jnp.logical_and(h == 0, t > 0))
        def _():
            for p in parts:
                halo_high(p).start()

    loads[1].wait()
    for c in loads[2:]:
        c.start()

    def logits_of(v):
        normed = rms_scale(v.astype(F32), ngain_ref[...]).astype(BF)
        return jnp.dot(normed, keys[...], preferred_element_type=F32)

    def softmax_of(l):
        e = jnp.exp(l - jnp.max(l, axis=-1, keepdims=True))
        return (e / jnp.sum(e, axis=-1, keepdims=True)).astype(BF)

    def first(r, peak):
        v = cells[pl.ds(3 + 2 * r, 2)].reshape(256, width)
        l = logits_of(v)
        logits[pl.ds(2 * r, 2)] = l.reshape(2, 128, width)
        return jnp.maximum(peak, jnp.max(l.reshape(32, 8, width), axis=0))

    def wait_low():
        @pl.when(t > 0)
        def _():
            for p in range(3):
                halo_low(p).wait_recv()

    def wait_high():
        @pl.when(t < nt - 1)
        def _():
            for p in range(3):
                halo_high(p).wait_recv()

    def halo_combine(cross):
        if cross:
            pl.when(h == 0)(wait_low)
            pl.when(h == 1)(wait_high)
            at = pl.ds(11 * h, 3)
        else:
            pl.when(h == 1)(wait_low)
            pl.when(h == 0)(wait_high)
            at = pl.ds(11 * (1 - h), 3)
        combine[at] = softmax_of(logits_of(cells[at].reshape(384, width))).reshape(3, 128, width)

    peak = lax.fori_loop(0, 4, first, jnp.full((8, width), -jnp.inf, F32))
    mine = jnp.max(peak, axis=0, keepdims=True)
    peaks[x] = mine
    peak_copies = []
    for d in range(1, 4):
        k = lax.rem(x + d, 4)
        c = remote(peaks.at[x], peaks.at[x], peak_ss.at[d - 1], peak_rs.at[d - 1], at_tok(k * 2 + h))
        c.start()
        peak_copies.append(c)

    @pl.when(t == 0)
    def _():
        cells[pl.ds(0, 3)] = jnp.zeros((3, 128, width), BF)

    @pl.when(t == nt - 1)
    def _():
        cells[pl.ds(11, 3)] = jnp.zeros((3, 128, width), BF)


    @pl.loop(0, 8)
    def _(r):
        shifted = jnp.exp(logits[r] - mine)
        disp[:, pl.ds(pl.multiple_of(r * 128, 128), 128)] = shifted.T.astype(BF)

    @pl.loop(0, 8)
    def _(r):
        combine[3 + r] = softmax_of(logits[r])

    for c in peak_copies:
        c.wait_recv()
    top = jnp.maximum(jnp.maximum(peaks[0], peaks[1]), jnp.maximum(peaks[2], peaks[3]))
    tops[h] = top
    top_copy = remote(tops.at[h], tops.at[h], top_ss, top_rs, to_pair)
    top_copy.start()

    def as_column(row):
        return jnp.broadcast_to(row, (128, width)).T

    shrink[...] = as_column(jnp.exp(mine - top)).reshape(nf, 4, 16, 128)

    w_copies, x_copies = [], []

    def pass_on(n):
        lane = pl.ds(n * cw, cw)
        for c in w_copies[n]:
            c.wait_recv()
        numer[0:8, right, :, lane] = (
            numer[0:8, right, :, lane].astype(F32) + passed[0, :, :, lane].astype(F32)
        ).astype(BF)
        numer[8:16, left, :, lane] = (
            numer[8:16, left, :, lane].astype(F32) + passed[1, :, :, lane].astype(F32)
        ).astype(BF)
        row = [
            remote(numer.at[:, right, :, lane], rx.at[0, :, :, lane], x_ss.at[n, 0], x_rs.at[n, 0], to_right),
            remote(numer.at[:, left, :, lane], rx.at[1, :, :, lane], x_ss.at[n, 1], x_rs.at[n, 1], to_left),
        ]
        for c in row:
            c.start()
        x_copies.append(row)

    for n in range(NCH):
        lane = pl.ds(n * cw, cw)
        own = cells[pl.ds(3, 8), :, lane].reshape(1024, cw)
        factor = shrink[...].reshape(1024, 128)
        numer[:, :, :, lane] = (
            jnp.dot(disp[...], own, preferred_element_type=F32) * jnp.concatenate([factor] * (cw // 128), axis=1)
        ).astype(BF).reshape(nf, 4, 16, cw)
        low = pl.ds(0, 8)
        high = pl.ds(8, 8)
        row = [
            remote(
                numer.at[low, across, :, lane], passed.at[0, :, :, lane], w_ss.at[n, 0], w_rs.at[n, 0], to_right
            ),
            remote(
                numer.at[high, across, :, lane], passed.at[1, :, :, lane], w_ss.at[n, 1], w_rs.at[n, 1], to_left
            ),
        ]
        for c in row:
            c.start()
        w_copies.append(row)
        if n > 0:
            pass_on(n - 1)
    pass_on(NCH - 1)

    y_copies = []
    for n in range(NCH):
        lane = pl.ds(n * cw, cw)
        for c in x_copies[n]:
            c.wait_recv()
        total = numer[:, x, :, lane].astype(F32)
        for d in range(2):
            total = total + rx[d, :, :, lane].astype(F32)
        low = total[:, 0:8].reshape(nf * 8, cw)
        high = total[:, 8:16].reshape(nf * 8, cw)
        ysend[:, lane] = jnp.where(h == 0, high, low).astype(BF)
        keep[:, lane] = jnp.where(h == 0, low, high)
        c = remote(ysend.at[:, lane], yrecv.at[:, lane], y_ss.at[n], y_rs.at[n], to_pair)
        c.start()
        y_copies.append(c)

    top_copy.wait_recv()
    whole = jnp.maximum(tops[0], tops[1])

    def my_slots(row):
        shrink[...] = as_column(row).reshape(nf, 4, 16, 128)
        both = shrink[:, x]
        picked = jnp.where(h == 0, both[:, 0:8], both[:, 8:16]).reshape(nf * 8, 128)
        return jnp.concatenate([picked] * (width // 128), axis=1)

    keep[...] = keep[...] * my_slots(jnp.exp(tops[h] - whole))
    other = my_slots(jnp.exp(tops[1 - h] - whole))
    for c in y_copies:
        c.wait_recv()
    local_in = rms_scale(keep[...] + yrecv[...].astype(F32) * other, sgain_ref[...])
    asend[...] = fold_halves(local_in.reshape(nf, 8, width)).astype(BF)
    arecv[f] = asend[f]
    a_copies = []
    for d in range(1, nf):
        k = lax.rem(f + d, nf)
        c = remote(asend.at[k], arecv.at[f], a_ss.at[d - 1], a_rs.at[d - 1], at_fc(k))
        c.start()
        a_copies.append(c)
    start_cross(AT_SEND)
    halo_combine(False)
    loads[2].wait()
    loads[3].wait()
    for c in a_copies:
        c.wait_recv()

    lhs = unfold_halves(arecv[...].astype(F32)).reshape(nf * 8, width).astype(BF)
    which = lax.rem(lax.broadcasted_iota(jnp.int32, (nf * 8, 1), 0), 8) < 4
    hid = jnp.where(
        which,
        jnp.dot(lhs, win[0], preferred_element_type=F32),
        jnp.dot(lhs, win[1], preferred_element_type=F32),
    )
    hid = jax.nn.gelu(hid).astype(BF)
    out = jnp.where(
        which,
        jnp.dot(hid, wout[0], preferred_element_type=F32),
        jnp.dot(hid, wout[1], preferred_element_type=F32),
    )
    bsend[...] = out.reshape(nf, 8, width).astype(BF)
    every[t, f] = bsend[f]
    b_copies = []
    for d in range(1, nf):
        k = lax.rem(f + d, nf)
        c = remote(bsend.at[k], every.at[t, f], b_ss.at[d - 1], b_rs.at[d - 1], at_fc(k))
        c.start()
        b_copies.append(c)
    start_cross(AT_RETURN)
    for c in b_copies:
        c.wait_recv()

    sides = ((h, t), (1 - h, x * 2 + 1 - h))
    pair_copies = []
    for n in range(NCH):
        ref = every.at[t, :, :, pl.ds(n * cw, cw)]
        c = remote(ref, ref, p_ss.at[n], p_rs.at[n], to_pair)
        c.start()
        pair_copies.append(c)
    g_copies, o_copies = {}, {}

    def send_out(b, n):
        if b == 1:
            pair_copies[n].wait_recv()
        ref = every.at[sides[b][1], :, :, pl.ds(n * cw, cw)]
        g_copies[b, n] = [
            remote(ref, ref, g_ss.at[b, n, 0], g_rs.at[b, n, 0], to_right),
            remote(ref, ref, g_ss.at[b, n, 1], g_rs.at[b, n, 1], to_left),
        ]
        for c in g_copies[b, n]:
            c.start()

    def forward(b, n):
        lane = pl.ds(n * cw, cw)
        g_copies[b, n][0].wait_recv()
        ref = every.at[left * 2 + sides[b][0], pl.ds(0, 8), :, lane]
        go = remote(ref, ref, o_ss.at[b, n, 0], o_rs.at[b, n, 0], to_right)
        go.start()
        g_copies[b, n][1].wait_recv()
        ref = every.at[right * 2 + sides[b][0], pl.ds(8, 8), :, lane]
        back = remote(ref, ref, o_ss.at[b, n, 1], o_rs.at[b, n, 1], to_left)
        back.start()
        o_copies[b, n] = [go, back]

    rows = 7 * 128

    def mix(n):
        lane = pl.ds(n * cw, cw)
        for b in range(2):
            for c in o_copies[b, n]:
                c.wait_recv()
        joined[...] = jnp.concatenate(
            [every[tt, ff, :, lane].astype(F32) for ff in range(nf) for tt in range(nt)], axis=0
        ).astype(BF)

        @pl.loop(0, 2)
        def _(b):
            mixed = jnp.dot(
                combine[pl.ds(b * 7, 7)].reshape(rows, width), joined[...], preferred_element_type=F32
            )
            v = cells[pl.ds(b * 7, 7), :, lane].reshape(rows, cw).astype(F32) + mixed
            at = lax.broadcasted_iota(jnp.int32, (rows, 1), 0) + (b * rows + (8 * t - 3) * 128)
            inside = jnp.logical_and(at >= 0, at < 64 * 128)
            v = jnp.where(inside, v, 0.0)
            state[pl.ds(b * 7, 7), :, lane] = v.astype(BF).reshape(7, 128, cw)

    def convolve(k):
        lane = pl.ds(k * 128, 128)
        for tap in range(49):
            row = cw_ref[tap // 7, pl.ds(tap % 7, 1), lane]
            taps[tap] = jnp.broadcast_to(row, (16, 128)).astype(BF)

        @pl.loop(0, 14)
        def _(r):
            v = state[r, :, lane].astype(F32)
            wide[r, pl.ds(8, 128), :] = v
            wide[r, pl.ds(0, 8), :] = v[120:128]
            wide[r, pl.ds(136, 8), :] = v[0:8]

        @pl.loop(0, 8)
        def _(i):
            acc = [[None] * 4, [None] * 4]
            for b in range(7):
                wv = [taps[a * 7 + b] for a in range(7)]
                for blk in range(2):
                    start = i * 16 + (8 * blk + 5 + b)
                    v = [wide[r, pl.ds(start, 8), :] for r in range(14)]
                    pk = [jnp.concatenate([v[q], v[q + 4]], axis=0).astype(BF) for q in range(10)]
                    for p in range(4):
                        term = tree_sum(pk[p + a] * wv[a] for a in range(7))
                        acc[blk][p] = term if acc[blk][p] is None else acc[blk][p] + term
            for blk in range(2):
                for p in range(4):
                    val = acc[blk][p].astype(F32)
                    at = pl.multiple_of(i * 16 + 8 * blk, 8)
                    conv[p, pl.ds(at, 8), lane] = val[0:8]
                    conv[p + 4, pl.ds(at, 8), lane] = val[8:16]

    send_out(0, 0)
    send_out(0, 1)
    start_cross(LATE)
    send_out(1, 0)
    forward(0, 0)
    send_out(0, 2)
    send_out(1, 1)
    forward(1, 0)
    forward(0, 1)
    halo_combine(True)
    mix(0)
    send_out(0, 3)
    send_out(1, 2)
    forward(1, 1)
    forward(0, 2)
    convolve(0)
    send_out(1, 3)
    forward(1, 2)
    forward(0, 3)
    convolve(1)
    mix(1)
    forward(1, 3)
    convolve(2)
    convolve(3)
    mix(2)
    convolve(4)
    convolve(5)
    mix(3)
    convolve(6)
    convolve(7)
    loads[4].wait()

    def norm_row(r, into):
        c = conv[r]
        center = c - jnp.mean(c, axis=-1, keepdims=True)
        spread = jnp.mean(center * center, axis=-1, keepdims=True)
        into[...] = (center * lax.rsqrt(spread + 1e-06) * lgain_ref[...]).astype(BF)

    def finish_row(r, source):
        branch = jnp.dot(source[...], proj[...], preferred_element_type=F32)
        res = state[r + 3].astype(F32) + scale_ref[...] * jax.nn.gelu(branch)
        outs[r] = res.astype(BF)
        pltpu.make_async_copy(outs.at[r], out_hbm.at[r], out_sem.at[r]).start()

    norm_row(0, even)

    @pl.loop(0, 4)
    def _(i):
        norm_row(2 * i + 1, odd)
        finish_row(2 * i, even)
        norm_row(jnp.minimum(2 * i + 2, 7), even)
        finish_row(2 * i + 1, odd)

    sent = peak_copies + y_copies + a_copies + b_copies + pair_copies + [top_copy]
    for group in (w_copies, x_copies, g_copies.values(), o_copies.values()):
        sent += [c for row in group for c in row]
    for c in sent:
        c.wait_send()

    @pl.when(t < nt - 1)
    def _():
        for p in range(3):
            halo_low(p).wait_send()

    @pl.when(t > 0)
    def _():
        for p in range(3):
            halo_high(p).wait_send()

    for r in range(8):
        pltpu.make_async_copy(outs.at[r], out_hbm.at[r], out_sem.at[r]).wait()


def fused(
    tokens, slot_keys, norm_gain, slot_gain, w_in, w_out, conv_weight, ln_gain, proj, layer_scale
):
    width = tokens.shape[2]
    vm = pl.BlockSpec(memory_space=pltpu.VMEM)
    anyspec = pl.BlockSpec(memory_space=pl.ANY)
    dma = pltpu.SemaphoreType.DMA
    nf = MEMBERS_AX
    return pl.pallas_call(
        mix_kernel,
        out_shape=jax.ShapeDtypeStruct((8, 128, width), BF),
        in_specs=[anyspec, anyspec, vm, vm, anyspec, anyspec, vm, vm, vm, anyspec],
        out_specs=anyspec,
        scratch_shapes=[
            pltpu.VMEM((14, 128, width), BF),
            pltpu.VMEM((width, width), BF),
            pltpu.VMEM(w_in.shape, BF),
            pltpu.VMEM(w_out.shape, BF),
            pltpu.VMEM((8, 128, width), F32),
            pltpu.VMEM((14, 128, width), BF),
            pltpu.VMEM((width, 1024), BF),
            pltpu.VMEM((nf, 4, 16, width), BF),
            pltpu.VMEM((2, 8, 16, width), BF),
            pltpu.VMEM((2, nf, 16, width), BF),
            pltpu.VMEM((nf * 8, width), BF),
            pltpu.VMEM((nf * 8, width), BF),
            pltpu.VMEM((nf * 8, width), F32),
            pltpu.VMEM((nf, 16, width // 2), BF),
            pltpu.VMEM((nf, 16, width // 2), BF),
            pltpu.VMEM((nf, 8, width), BF),
            pltpu.VMEM((8, nf, 8, width), BF),
            pltpu.VMEM((1024, width // NCH), BF),
            pltpu.VMEM((14, 128, width), BF),
            pltpu.VMEM((14, 144, 128), F32),
            pltpu.VMEM((49, 16, 128), BF),
            pltpu.VMEM((8, 128, width), F32),
            pltpu.VMEM((128, width), BF),
            pltpu.VMEM((128, width), BF),
            pltpu.VMEM((8, 128, width), BF),
            pltpu.VMEM((width, width), BF),
            pltpu.VMEM((4, 1, width), F32),
            pltpu.VMEM((2, 1, width), F32),
            pltpu.VMEM((nf, 4, 16, 128), F32),
            dma((5,)),
            dma((3,)), dma((3,)),
            dma, dma,
            dma((2, 3)), dma((2, 3)),
            dma((NCH, 2)), dma((NCH, 2)),
            dma((NCH, 2)), dma((NCH, 2)),
            dma((NCH,)), dma((NCH,)),
            dma((15,)), dma((15,)),
            dma((15,)), dma((15,)),
            dma((NCH,)), dma((NCH,)),
            dma((2, NCH, 2)), dma((2, NCH, 2)),
            dma((2, NCH, 2)), dma((2, NCH, 2)),
            dma((8,)),
        ],
        compiler_params=pltpu.CompilerParams(
            collective_id=0, has_side_effects=True, vmem_limit_bytes=62 * 1024 * 1024
        ),
        name="fused",
    )(
        tokens, slot_keys, norm_gain.reshape(1, width), slot_gain.reshape(1, width), w_in, w_out,
        conv_weight, ln_gain.reshape(1, width), layer_scale.reshape(1, width), proj,
    )


def tree_sum(terms):
    terms = list(terms)
    while len(terms) > 1:
        nxt = [terms[i] + terms[i + 1] for i in range(0, len(terms) - 1, 2)]
        if len(terms) % 2:
            nxt.append(terms[-1])
        terms = nxt
    return terms[0]


def local(
    tokens, slot_keys, norm_gain, slot_gain, w_in, w_out, conv_weight, ln_gain, proj, layer_scale
):
    return fused(
        tokens[0], slot_keys, norm_gain, slot_gain, w_in, w_out, conv_weight, ln_gain, proj, layer_scale
    )[None]


def solution(mesh):
    in_specs = (
        P("fc", "tok", None, None),
        P(),
        P(),
        P(),
        P(("fc", "tok"), None, None),
        P(("fc", "tok"), None, None),
        P(),
        P(),
        P(),
        P(),
    )
    out_specs = P("fc", "tok", None, None)
    return jax.shard_map(local, mesh=mesh, in_specs=in_specs, out_specs=out_specs, check_vma=False)
```

```python
import jax
import jax.numpy as jnp
from jax import lax
from jax.experimental import pallas as pl
from jax.experimental.pallas import tpu as pltpu
from jax.sharding import PartitionSpec as P

BF = jnp.bfloat16
F32 = jnp.float32
MESH = pl.DeviceIdType.MESH
MEMBERS_AX = 16
NCH = 4
FIRST, EARLY, AT_EXPERT, LATE = (0,), (1,), (), (2,)


def rms_scale(value, gain):
    return value * lax.rsqrt(jnp.mean(value * value, axis=-1, keepdims=True) + 1e-06) * gain


def fold_halves(v):
    half = v.shape[-1] // 2
    return jnp.concatenate([v[..., :half], v[..., half:]], axis=-2)


def unfold_halves(v):
    rows = v.shape[-2] // 2
    return jnp.concatenate([v[..., :rows, :], v[..., rows:, :]], axis=-1)


def mix_kernel(
    tok_hbm, keys_hbm, ngain_ref, sgain_ref, win_hbm, wout_hbm, cw_ref, lgain_ref, scale_ref, proj_hbm,
    out_hbm,
    cells, keys, win, wout, logits, combine, disp, numer, passed, rx, ysend, yrecv, keep,
    asend, arecv, bsend, every, joined, state, wide, taps, conv, even, odd, outs, proj, peaks, tops, shrink, load_sem,
    peak_ss, peak_rs, top_ss, top_rs, halo_ss, halo_rs, w_ss, w_rs, x_ss, x_rs, y_ss, y_rs, a_ss, a_rs, b_ss, b_rs,
    p_ss, p_rs, g_ss, g_rs, out_sem,
):
    nf, nt = MEMBERS_AX, 8
    width = cells.shape[2]
    cw = width // NCH
    f = lax.axis_index("fc")
    t = lax.axis_index("tok")
    x = lax.div(t, 2)
    h = lax.rem(t, 2)

    def at_tok(k):
        return {"fc": f, "tok": k}

    def at_fc(k):
        return {"fc": k, "tok": t}

    right, left, across = lax.rem(x + 1, 4), lax.rem(x + 3, 4), lax.rem(x + 2, 4)
    to_right, to_left, to_pair = at_tok(right * 2 + h), at_tok(left * 2 + h), at_tok(x * 2 + 1 - h)

    loads = [
        pltpu.make_async_copy(tok_hbm, cells.at[pl.ds(3, 8)], load_sem.at[0]),
        pltpu.make_async_copy(keys_hbm, keys, load_sem.at[1]),
        pltpu.make_async_copy(win_hbm, win, load_sem.at[2]),
        pltpu.make_async_copy(wout_hbm, wout, load_sem.at[3]),
        pltpu.make_async_copy(proj_hbm, proj, load_sem.at[4]),
    ]
    loads[0].start()
    loads[1].start()

    barrier = pltpu.get_barrier_semaphore()
    for d in range(1, nt):
        pl.semaphore_signal(barrier, inc=1, device_id=at_tok(lax.rem(t + d, nt)), device_id_type=MESH)
    for d in range(1, nf):
        pl.semaphore_signal(barrier, inc=1, device_id=at_fc(lax.rem(f + d, nf)), device_id_type=MESH)

    def remote(src, dst, ss, rs, dev):
        return pltpu.make_async_remote_copy(
            src_ref=src, dst_ref=dst, send_sem=ss, recv_sem=rs, device_id=dev, device_id_type=MESH
        )

    loads[0].wait()

    def halo_low(p):
        return remote(
            cells.at[8 + p], cells.at[p], halo_ss.at[0, p], halo_rs.at[0, p], at_tok(t + 1)
        )

    def halo_high(p):
        return remote(
            cells.at[3 + p], cells.at[11 + p], halo_ss.at[1, p], halo_rs.at[1, p], at_tok(t - 1)
        )

    def start_cross(parts):
        @pl.when(jnp.logical_and(h == 1, t < nt - 1))
        def _():
            for p in parts:
                halo_low(p).start()

        @pl.when(jnp.logical_and(h == 0, t > 0))
        def _():
            for p in parts:
                halo_high(p).start()

    loads[1].wait()
    for c in loads[2:]:
        c.start()

    def logits_of(v):
        normed = rms_scale(v.astype(F32), ngain_ref[...]).astype(BF)
        return jnp.dot(normed, keys[...], preferred_element_type=F32)

    def softmax_of(l):
        e = jnp.exp(l - jnp.max(l, axis=-1, keepdims=True))
        return (e / jnp.sum(e, axis=-1, keepdims=True)).astype(BF)

    def first(r, peak):
        v = cells[pl.ds(3 + 2 * r, 2)].reshape(256, width)
        l = logits_of(v)
        logits[pl.ds(2 * r, 2)] = l.reshape(2, 128, width)
        return jnp.maximum(peak, jnp.max(l.reshape(32, 8, width), axis=0))

    def halo_combine(cross, start, count):
        def wait_low():
            @pl.when(t > 0)
            def _():
                for p in range(start, start + count):
                    halo_low(p).wait_recv()

        def wait_high():
            @pl.when(t < nt - 1)
            def _():
                for p in range(start, start + count):
                    halo_high(p).wait_recv()

        pl.when(h == (0 if cross else 1))(wait_low)
        pl.when(h == (1 if cross else 0))(wait_high)
        at = pl.ds(11 * (h if cross else 1 - h) + start, count)
        rows_in = cells[at].reshape(count * 128, width)
        combine[at] = softmax_of(logits_of(rows_in)).reshape(count, 128, width)

    peak = lax.fori_loop(0, 2, first, jnp.full((8, width), -jnp.inf, F32))
    pl.semaphore_wait(barrier, nt + nf - 2)

    start_cross(FIRST)
    peak = lax.fori_loop(2, 4, first, peak)
    mine = jnp.max(peak, axis=0, keepdims=True)
    peaks[x] = mine
    peak_copies = []
    for d in range(1, 4):
        k = lax.rem(x + d, 4)
        c = remote(peaks.at[x], peaks.at[x], peak_ss.at[d - 1], peak_rs.at[d - 1], at_tok(k * 2 + h))
        c.start()
        peak_copies.append(c)

    @pl.when(h == 0)
    def _():
        for p in range(3):
            halo_low(p).start()

    @pl.when(h == 1)
    def _():
        for p in range(3):
            halo_high(p).start()

    @pl.when(t == 0)
    def _():
        cells[pl.ds(0, 3)] = jnp.zeros((3, 128, width), BF)

    @pl.when(t == nt - 1)
    def _():
        cells[pl.ds(11, 3)] = jnp.zeros((3, 128, width), BF)


    @pl.loop(0, 8)
    def _(r):
        shifted = jnp.exp(logits[r] - mine)
        disp[:, pl.ds(pl.multiple_of(r * 128, 128), 128)] = shifted.T.astype(BF)

    @pl.loop(0, 8)
    def _(r):
        combine[3 + r] = softmax_of(logits[r])

    for c in peak_copies:
        c.wait_recv()
    start_cross(EARLY)
    top = jnp.maximum(jnp.maximum(peaks[0], peaks[1]), jnp.maximum(peaks[2], peaks[3]))
    tops[h] = top
    top_copy = remote(tops.at[h], tops.at[h], top_ss, top_rs, to_pair)
    top_copy.start()

    def as_column(row):
        return jnp.broadcast_to(row, (128, width)).T

    shrink[...] = as_column(jnp.exp(mine - top)).reshape(nf, 4, 16, 128)

    w_copies, x_copies = [], []

    def pass_on(n):
        lane = pl.ds(n * cw, cw)
        for c in w_copies[n]:
            c.wait_recv()
        numer[0:8, right, :, lane] = (
            numer[0:8, right, :, lane].astype(F32) + passed[0, :, :, lane].astype(F32)
        ).astype(BF)
        numer[8:16, left, :, lane] = (
            numer[8:16, left, :, lane].astype(F32) + passed[1, :, :, lane].astype(F32)
        ).astype(BF)
        row = [
            remote(numer.at[:, right, :, lane], rx.at[0, :, :, lane], x_ss.at[n, 0], x_rs.at[n, 0], to_right),
            remote(numer.at[:, left, :, lane], rx.at[1, :, :, lane], x_ss.at[n, 1], x_rs.at[n, 1], to_left),
        ]
        for c in row:
            c.start()
        x_copies.append(row)

    for n in range(NCH):
        lane = pl.ds(n * cw, cw)
        own = cells[pl.ds(3, 8), :, lane].reshape(1024, cw)
        factor = shrink[...].reshape(1024, 128)
        numer[:, :, :, lane] = (
            jnp.dot(disp[...], own, preferred_element_type=F32) * jnp.concatenate([factor] * (cw // 128), axis=1)
        ).astype(BF).reshape(nf, 4, 16, cw)
        low = pl.ds(0, 8)
        high = pl.ds(8, 8)
        row = [
            remote(
                numer.at[low, across, :, lane], passed.at[0, :, :, lane], w_ss.at[n, 0], w_rs.at[n, 0], to_right
            ),
            remote(
                numer.at[high, across, :, lane], passed.at[1, :, :, lane], w_ss.at[n, 1], w_rs.at[n, 1], to_left
            ),
        ]
        for c in row:
            c.start()
        w_copies.append(row)
        if n > 0:
            pass_on(n - 1)
    pass_on(NCH - 1)

    y_copies = []
    for n in range(NCH):
        lane = pl.ds(n * cw, cw)
        for c in x_copies[n]:
            c.wait_recv()
        total = numer[:, x, :, lane].astype(F32)
        for d in range(2):
            total = total + rx[d, :, :, lane].astype(F32)
        low = total[:, 0:8].reshape(nf * 8, cw)
        high = total[:, 8:16].reshape(nf * 8, cw)
        ysend[:, lane] = jnp.where(h == 0, high, low).astype(BF)
        keep[:, lane] = jnp.where(h == 0, low, high)
        c = remote(ysend.at[:, lane], yrecv.at[:, lane], y_ss.at[n], y_rs.at[n], to_pair)
        c.start()
        y_copies.append(c)

    top_copy.wait_recv()
    whole = jnp.maximum(tops[0], tops[1])

    def my_slots(row):
        shrink[...] = as_column(row).reshape(nf, 4, 16, 128)
        both = shrink[:, x]
        picked = jnp.where(h == 0, both[:, 0:8], both[:, 8:16]).reshape(nf * 8, 128)
        return jnp.concatenate([picked] * (width // 128), axis=1)

    keep[...] = keep[...] * my_slots(jnp.exp(tops[h] - whole))
    other = my_slots(jnp.exp(tops[1 - h] - whole))
    for c in y_copies:
        c.wait_recv()
    local_in = rms_scale(keep[...] + yrecv[...].astype(F32) * other, sgain_ref[...])
    asend[...] = fold_halves(local_in.reshape(nf, 8, width)).astype(BF)
    arecv[f] = asend[f]
    a_copies = []
    for d in range(1, nf):
        k = lax.rem(f + d, nf)
        c = remote(asend.at[k], arecv.at[f], a_ss.at[d - 1], a_rs.at[d - 1], at_fc(k))
        c.start()
        a_copies.append(c)
    halo_combine(False, 0, 3)
    loads[2].wait()
    loads[3].wait()
    for c in a_copies:
        c.wait_recv()

    start_cross(AT_EXPERT)
    lhs = unfold_halves(arecv[...].astype(F32)).reshape(nf * 8, width).astype(BF)
    which = lax.rem(lax.broadcasted_iota(jnp.int32, (nf * 8, 1), 0), 8) < 4
    hid = jnp.where(
        which,
        jnp.dot(lhs, win[0], preferred_element_type=F32),
        jnp.dot(lhs, win[1], preferred_element_type=F32),
    )
    hid = jax.nn.gelu(hid).astype(BF)
    out = jnp.where(
        which,
        jnp.dot(hid, wout[0], preferred_element_type=F32),
        jnp.dot(hid, wout[1], preferred_element_type=F32),
    )
    bsend[...] = out.reshape(nf, 8, width).astype(BF)
    every[t, f] = bsend[f]
    b_copies = []
    for d in range(1, nf):
        k = lax.rem(f + d, nf)
        c = remote(bsend.at[k], every.at[t, f], b_ss.at[d - 1], b_rs.at[d - 1], at_fc(k))
        c.start()
        b_copies.append(c)
    halo_combine(True, 0, 2)
    for c in b_copies:
        c.wait_recv()

    sides = ((h, t), (1 - h, x * 2 + 1 - h))
    pair_copies = []
    for n in range(NCH):
        ref = every.at[t, :, :, pl.ds(n * cw, cw)]
        c = remote(ref, ref, p_ss.at[n], p_rs.at[n], to_pair)
        c.start()
        pair_copies.append(c)
        if n == 1:
            start_cross(LATE)
    g_copies = {}

    def send_out(b, n):
        if b == 1:
            pair_copies[n].wait_recv()
        ref = every.at[sides[b][1], :, :, pl.ds(n * cw, cw)]
        g_copies[b, n] = []
        for d in (1, 3, 2):
            c = remote(
                ref, ref, g_ss.at[b, n, d - 1], g_rs.at[b, n, d - 1], at_tok(lax.rem(x + d, 4) * 2 + h)
            )
            c.start()
            g_copies[b, n].append(c)

    rows = 7 * 128

    def mix(n):
        lane = pl.ds(n * cw, cw)
        for c in g_copies[0, n] + g_copies[1, n]:
            c.wait_recv()
        joined[...] = jnp.concatenate(
            [every[tt, ff, :, lane].astype(F32) for ff in range(nf) for tt in range(nt)], axis=0
        ).astype(BF)

        @pl.loop(0, 2)
        def _(b):
            mixed = jnp.dot(
                combine[pl.ds(b * 7, 7)].reshape(rows, width), joined[...], preferred_element_type=F32
            )
            v = cells[pl.ds(b * 7, 7), :, lane].reshape(rows, cw).astype(F32) + mixed
            at = lax.broadcasted_iota(jnp.int32, (rows, 1), 0) + (b * rows + (8 * t - 3) * 128)
            inside = jnp.logical_and(at >= 0, at < 64 * 128)
            v = jnp.where(inside, v, 0.0)
            state[pl.ds(b * 7, 7), :, lane] = v.astype(BF).reshape(7, 128, cw)

    def convolve(k):
        lane = pl.ds(k * 128, 128)
        for tap in range(49):
            row = cw_ref[tap // 7, pl.ds(tap % 7, 1), lane]
            taps[tap] = jnp.broadcast_to(row, (16, 128)).astype(BF)

        @pl.loop(0, 14)
        def _(r):
            v = state[r, :, lane].astype(F32)
            wide[r, pl.ds(8, 128), :] = v
            wide[r, pl.ds(0, 8), :] = v[120:128]
            wide[r, pl.ds(136, 8), :] = v[0:8]

        @pl.loop(0, 8)
        def _(i):
            acc = [[None] * 4, [None] * 4]
            for b in range(7):
                wv = [taps[a * 7 + b] for a in range(7)]
                for blk in range(2):
                    start = i * 16 + (8 * blk + 5 + b)
                    v = [wide[r, pl.ds(start, 8), :] for r in range(14)]
                    pk = [jnp.concatenate([v[q], v[q + 4]], axis=0).astype(BF) for q in range(10)]
                    for p in range(4):
                        term = tree_sum(pk[p + a] * wv[a] for a in range(7))
                        acc[blk][p] = term if acc[blk][p] is None else acc[blk][p] + term
            for blk in range(2):
                for p in range(4):
                    val = acc[blk][p].astype(F32)
                    at = pl.multiple_of(i * 16 + 8 * blk, 8)
                    conv[p, pl.ds(at, 8), lane] = val[0:8]
                    conv[p + 4, pl.ds(at, 8), lane] = val[8:16]

    send_out(0, 0)
    send_out(0, 1)
    send_out(1, 0)
    send_out(1, 1)
    send_out(0, 2)
    halo_combine(True, 2, 1)
    send_out(1, 2)
    send_out(0, 3)
    send_out(1, 3)
    mix(0)
    convolve(0)
    convolve(1)
    mix(1)
    convolve(2)
    convolve(3)
    mix(2)
    convolve(4)
    convolve(5)
    mix(3)
    convolve(6)
    convolve(7)
    loads[4].wait()

    def norm_row(r, into):
        c = conv[r]
        center = c - jnp.mean(c, axis=-1, keepdims=True)
        spread = jnp.mean(center * center, axis=-1, keepdims=True)
        into[...] = (center * lax.rsqrt(spread + 1e-06) * lgain_ref[...]).astype(BF)

    def finish_row(r, source):
        branch = jnp.dot(source[...], proj[...], preferred_element_type=F32)
        res = state[r + 3].astype(F32) + scale_ref[...] * jax.nn.gelu(branch)
        outs[r] = res.astype(BF)
        pltpu.make_async_copy(outs.at[r], out_hbm.at[r], out_sem.at[r]).start()

    norm_row(0, even)

    @pl.loop(0, 4)
    def _(i):
        norm_row(2 * i + 1, odd)
        finish_row(2 * i, even)
        norm_row(jnp.minimum(2 * i + 2, 7), even)
        finish_row(2 * i + 1, odd)

    sent = peak_copies + y_copies + a_copies + b_copies + pair_copies + [top_copy]
    for group in (w_copies, x_copies, g_copies.values()):
        sent += [c for row in group for c in row]
    for c in sent:
        c.wait_send()

    @pl.when(t < nt - 1)
    def _():
        for p in range(3):
            halo_low(p).wait_send()

    @pl.when(t > 0)
    def _():
        for p in range(3):
            halo_high(p).wait_send()

    for r in range(8):
        pltpu.make_async_copy(outs.at[r], out_hbm.at[r], out_sem.at[r]).wait()


def fused(
    tokens, slot_keys, norm_gain, slot_gain, w_in, w_out, conv_weight, ln_gain, proj, layer_scale
):
    width = tokens.shape[2]
    vm = pl.BlockSpec(memory_space=pltpu.VMEM)
    anyspec = pl.BlockSpec(memory_space=pl.ANY)
    dma = pltpu.SemaphoreType.DMA
    nf = MEMBERS_AX
    return pl.pallas_call(
        mix_kernel,
        out_shape=jax.ShapeDtypeStruct((8, 128, width), BF),
        in_specs=[anyspec, anyspec, vm, vm, anyspec, anyspec, vm, vm, vm, anyspec],
        out_specs=anyspec,
        scratch_shapes=[
            pltpu.VMEM((14, 128, width), BF),
            pltpu.VMEM((width, width), BF),
            pltpu.VMEM(w_in.shape, BF),
            pltpu.VMEM(w_out.shape, BF),
            pltpu.VMEM((8, 128, width), F32),
            pltpu.VMEM((14, 128, width), BF),
            pltpu.VMEM((width, 1024), BF),
            pltpu.VMEM((nf, 4, 16, width), BF),
            pltpu.VMEM((2, 8, 16, width), BF),
            pltpu.VMEM((2, nf, 16, width), BF),
            pltpu.VMEM((nf * 8, width), BF),
            pltpu.VMEM((nf * 8, width), BF),
            pltpu.VMEM((nf * 8, width), F32),
            pltpu.VMEM((nf, 16, width // 2), BF),
            pltpu.VMEM((nf, 16, width // 2), BF),
            pltpu.VMEM((nf, 8, width), BF),
            pltpu.VMEM((8, nf, 8, width), BF),
            pltpu.VMEM((1024, width // NCH), BF),
            pltpu.VMEM((14, 128, width), BF),
            pltpu.VMEM((14, 144, 128), F32),
            pltpu.VMEM((49, 16, 128), BF),
            pltpu.VMEM((8, 128, width), F32),
            pltpu.VMEM((128, width), BF),
            pltpu.VMEM((128, width), BF),
            pltpu.VMEM((8, 128, width), BF),
            pltpu.VMEM((width, width), BF),
            pltpu.VMEM((4, 1, width), F32),
            pltpu.VMEM((2, 1, width), F32),
            pltpu.VMEM((nf, 4, 16, 128), F32),
            dma((5,)),
            dma((3,)), dma((3,)),
            dma, dma,
            dma((2, 3)), dma((2, 3)),
            dma((NCH, 2)), dma((NCH, 2)),
            dma((NCH, 2)), dma((NCH, 2)),
            dma((NCH,)), dma((NCH,)),
            dma((15,)), dma((15,)),
            dma((15,)), dma((15,)),
            dma((NCH,)), dma((NCH,)),
            dma((2, NCH, 3)), dma((2, NCH, 3)),
            dma((8,)),
        ],
        compiler_params=pltpu.CompilerParams(
            collective_id=0, has_side_effects=True, vmem_limit_bytes=62 * 1024 * 1024
        ),
        name="fused",
    )(
        tokens, slot_keys, norm_gain.reshape(1, width), slot_gain.reshape(1, width), w_in, w_out,
        conv_weight, ln_gain.reshape(1, width), layer_scale.reshape(1, width), proj,
    )


def tree_sum(terms):
    terms = list(terms)
    while len(terms) > 1:
        nxt = [terms[i] + terms[i + 1] for i in range(0, len(terms) - 1, 2)]
        if len(terms) % 2:
            nxt.append(terms[-1])
        terms = nxt
    return terms[0]


def local(
    tokens, slot_keys, norm_gain, slot_gain, w_in, w_out, conv_weight, ln_gain, proj, layer_scale
):
    return fused(
        tokens[0], slot_keys, norm_gain, slot_gain, w_in, w_out, conv_weight, ln_gain, proj, layer_scale
    )[None]


def solution(mesh):
    in_specs = (
        P("fc", "tok", None, None),
        P(),
        P(),
        P(),
        P(("fc", "tok"), None, None),
        P(("fc", "tok"), None, None),
        P(),
        P(),
        P(),
        P(),
    )
    out_specs = P("fc", "tok", None, None)
    return jax.shard_map(local, mesh=mesh, in_specs=in_specs, out_specs=out_specs, check_vma=False)
```

```python
import jax
import jax.numpy as jnp
from jax import lax
from jax.experimental import pallas as pl
from jax.experimental.pallas import tpu as pltpu
from jax.sharding import PartitionSpec as P

BF = jnp.bfloat16
F32 = jnp.float32
MESH = pl.DeviceIdType.MESH
MEMBERS_AX = 16
NCH = 4
FIRST, EARLY, LAST = (2,), (1,), (0,)


def rms_scale(value, gain):
    return value * lax.rsqrt(jnp.mean(value * value, axis=-1, keepdims=True) + 1e-06) * gain


def fold_halves(v):
    half = v.shape[-1] // 2
    return jnp.concatenate([v[..., :half], v[..., half:]], axis=-2)


def unfold_halves(v):
    rows = v.shape[-2] // 2
    return jnp.concatenate([v[..., :rows, :], v[..., rows:, :]], axis=-1)


def mix_kernel(
    tok_hbm, keys_hbm, ngain_ref, sgain_ref, win_hbm, wout_hbm, cw_ref, lgain_ref, scale_ref, proj_hbm,
    out_hbm,
    cells, keys, win, wout, logits, combine, disp, numer, passed, rx, ysend, yrecv, keep,
    asend, arecv, bsend, every, joined, state, wide, taps, conv, even, odd, outs, proj, peaks, tops, shrink, load_sem,
    peak_ss, peak_rs, top_ss, top_rs, halo_ss, halo_rs, w_ss, w_rs, x_ss, x_rs, y_ss, y_rs, a_ss, a_rs, b_ss, b_rs,
    p_ss, p_rs, g_ss, g_rs, out_sem,
):
    nf, nt = MEMBERS_AX, 8
    width = cells.shape[2]
    cw = width // NCH
    f = lax.axis_index("fc")
    t = lax.axis_index("tok")
    x = lax.div(t, 2)
    h = lax.rem(t, 2)

    def at_tok(k):
        return {"fc": f, "tok": k}

    def at_fc(k):
        return {"fc": k, "tok": t}

    right, left, across = lax.rem(x + 1, 4), lax.rem(x + 3, 4), lax.rem(x + 2, 4)
    to_right, to_left, to_pair = at_tok(right * 2 + h), at_tok(left * 2 + h), at_tok(x * 2 + 1 - h)

    loads = [
        pltpu.make_async_copy(tok_hbm, cells.at[pl.ds(3, 8)], load_sem.at[0]),
        pltpu.make_async_copy(keys_hbm, keys, load_sem.at[1]),
        pltpu.make_async_copy(win_hbm, win, load_sem.at[2]),
        pltpu.make_async_copy(wout_hbm, wout, load_sem.at[3]),
        pltpu.make_async_copy(proj_hbm, proj, load_sem.at[4]),
    ]
    loads[0].start()
    loads[1].start()

    barrier = pltpu.get_barrier_semaphore()
    for d in range(1, nt):
        pl.semaphore_signal(barrier, inc=1, device_id=at_tok(lax.rem(t + d, nt)), device_id_type=MESH)
    for d in range(1, nf):
        pl.semaphore_signal(barrier, inc=1, device_id=at_fc(lax.rem(f + d, nf)), device_id_type=MESH)

    def remote(src, dst, ss, rs, dev):
        return pltpu.make_async_remote_copy(
            src_ref=src, dst_ref=dst, send_sem=ss, recv_sem=rs, device_id=dev, device_id_type=MESH
        )

    loads[0].wait()

    def halo_low(p):
        return remote(
            cells.at[8 + p], cells.at[p], halo_ss.at[0, p], halo_rs.at[0, p], at_tok(t + 1)
        )

    def halo_high(p):
        return remote(
            cells.at[3 + p], cells.at[11 + p], halo_ss.at[1, p], halo_rs.at[1, p], at_tok(t - 1)
        )

    def start_cross(parts):
        @pl.when(jnp.logical_and(h == 1, t < nt - 1))
        def _():
            for p in parts:
                halo_low(p).start()

        @pl.when(jnp.logical_and(h == 0, t > 0))
        def _():
            for p in parts:
                halo_high(2 - p).start()

    loads[1].wait()
    for c in loads[2:]:
        c.start()

    def logits_of(v):
        normed = rms_scale(v.astype(F32), ngain_ref[...]).astype(BF)
        return jnp.dot(normed, keys[...], preferred_element_type=F32)

    def softmax_of(l):
        e = jnp.exp(l - jnp.max(l, axis=-1, keepdims=True))
        return (e / jnp.sum(e, axis=-1, keepdims=True)).astype(BF)

    def first(r, peak):
        v = cells[pl.ds(3 + 2 * r, 2)].reshape(256, width)
        l = logits_of(v)
        logits[pl.ds(2 * r, 2)] = l.reshape(2, 128, width)
        return jnp.maximum(peak, jnp.max(l.reshape(32, 8, width), axis=0))

    def pure_combine():
        @pl.when(h == 1)
        def _():
            for p in range(3):
                halo_low(p).wait_recv()

        @pl.when(h == 0)
        def _():
            for p in range(3):
                halo_high(p).wait_recv()

        at = pl.ds(11 * (1 - h), 3)
        rows_in = cells[at].reshape(384, width)
        combine[at] = softmax_of(logits_of(rows_in)).reshape(3, 128, width)

    def cross_at(p):
        return p + h * (13 - 2 * p)

    def cross_combine(p):
        @pl.when(jnp.logical_and(h == 0, t > 0))
        def _():
            halo_low(p).wait_recv()

        @pl.when(jnp.logical_and(h == 1, t < nt - 1))
        def _():
            halo_high(2 - p).wait_recv()

        combine[cross_at(p)] = softmax_of(logits_of(cells[cross_at(p)]))

    peak = lax.fori_loop(0, 2, first, jnp.full((8, width), -jnp.inf, F32))
    pl.semaphore_wait(barrier, nt + nf - 2)

    start_cross(FIRST)
    peak = lax.fori_loop(2, 4, first, peak)
    mine = jnp.max(peak, axis=0, keepdims=True)
    peaks[x] = mine
    peak_copies = []
    for d in range(1, 4):
        k = lax.rem(x + d, 4)
        c = remote(peaks.at[x], peaks.at[x], peak_ss.at[d - 1], peak_rs.at[d - 1], at_tok(k * 2 + h))
        c.start()
        peak_copies.append(c)

    @pl.when(h == 0)
    def _():
        for p in range(3):
            halo_low(p).start()

    @pl.when(h == 1)
    def _():
        for p in range(3):
            halo_high(p).start()

    @pl.when(t == 0)
    def _():
        cells[pl.ds(0, 3)] = jnp.zeros((3, 128, width), BF)

    @pl.when(t == nt - 1)
    def _():
        cells[pl.ds(11, 3)] = jnp.zeros((3, 128, width), BF)


    @pl.loop(0, 8)
    def _(r):
        shifted = jnp.exp(logits[r] - mine)
        disp[:, pl.ds(pl.multiple_of(r * 128, 128), 128)] = shifted.T.astype(BF)

    @pl.loop(0, 8)
    def _(r):
        combine[3 + r] = softmax_of(logits[r])

    for c in peak_copies:
        c.wait_recv()
    start_cross(EARLY)
    top = jnp.maximum(jnp.maximum(peaks[0], peaks[1]), jnp.maximum(peaks[2], peaks[3]))
    tops[h] = top
    top_copy = remote(tops.at[h], tops.at[h], top_ss, top_rs, to_pair)
    top_copy.start()

    def as_column(row):
        return jnp.broadcast_to(row, (128, width)).T

    shrink[...] = as_column(jnp.exp(mine - top)).reshape(nf, 4, 16, 128)

    w_copies, x_copies = [], []

    def pass_on(n):
        lane = pl.ds(n * cw, cw)
        for c in w_copies[n]:
            c.wait_recv()
        numer[0:8, right, :, lane] = (
            numer[0:8, right, :, lane].astype(F32) + passed[0, :, :, lane].astype(F32)
        ).astype(BF)
        numer[8:16, left, :, lane] = (
            numer[8:16, left, :, lane].astype(F32) + passed[1, :, :, lane].astype(F32)
        ).astype(BF)
        row = [
            remote(numer.at[:, right, :, lane], rx.at[0, :, :, lane], x_ss.at[n, 0], x_rs.at[n, 0], to_right),
            remote(numer.at[:, left, :, lane], rx.at[1, :, :, lane], x_ss.at[n, 1], x_rs.at[n, 1], to_left),
        ]
        for c in row:
            c.start()
        x_copies.append(row)

    for n in range(NCH):
        lane = pl.ds(n * cw, cw)
        own = cells[pl.ds(3, 8), :, lane].reshape(1024, cw)
        factor = shrink[...].reshape(1024, 128)
        numer[:, :, :, lane] = (
            jnp.dot(disp[...], own, preferred_element_type=F32) * jnp.concatenate([factor] * (cw // 128), axis=1)
        ).astype(BF).reshape(nf, 4, 16, cw)
        low = pl.ds(0, 8)
        high = pl.ds(8, 8)
        row = [
            remote(
                numer.at[low, across, :, lane], passed.at[0, :, :, lane], w_ss.at[n, 0], w_rs.at[n, 0], to_right
            ),
            remote(
                numer.at[high, across, :, lane], passed.at[1, :, :, lane], w_ss.at[n, 1], w_rs.at[n, 1], to_left
            ),
        ]
        for c in row:
            c.start()
        w_copies.append(row)
        if n > 0:
            pass_on(n - 1)
    pass_on(NCH - 1)

    y_copies = []
    for n in range(NCH):
        lane = pl.ds(n * cw, cw)
        for c in x_copies[n]:
            c.wait_recv()
        total = numer[:, x, :, lane].astype(F32)
        for d in range(2):
            total = total + rx[d, :, :, lane].astype(F32)
        low = total[:, 0:8].reshape(nf * 8, cw)
        high = total[:, 8:16].reshape(nf * 8, cw)
        ysend[:, lane] = jnp.where(h == 0, high, low).astype(BF)
        keep[:, lane] = jnp.where(h == 0, low, high)
        c = remote(ysend.at[:, lane], yrecv.at[:, lane], y_ss.at[n], y_rs.at[n], to_pair)
        c.start()
        y_copies.append(c)

    top_copy.wait_recv()
    whole = jnp.maximum(tops[0], tops[1])

    def my_slots(row):
        shrink[...] = as_column(row).reshape(nf, 4, 16, 128)
        both = shrink[:, x]
        picked = jnp.where(h == 0, both[:, 0:8], both[:, 8:16]).reshape(nf * 8, 128)
        return jnp.concatenate([picked] * (width // 128), axis=1)

    keep[...] = keep[...] * my_slots(jnp.exp(tops[h] - whole))
    other = my_slots(jnp.exp(tops[1 - h] - whole))
    for c in y_copies:
        c.wait_recv()
    local_in = rms_scale(keep[...] + yrecv[...].astype(F32) * other, sgain_ref[...])
    asend[...] = fold_halves(local_in.reshape(nf, 8, width)).astype(BF)
    arecv[f] = asend[f]
    a_copies = []
    for d in range(1, nf):
        k = lax.rem(f + d, nf)
        c = remote(asend.at[k], arecv.at[f], a_ss.at[d - 1], a_rs.at[d - 1], at_fc(k))
        c.start()
        a_copies.append(c)
    pure_combine()
    loads[2].wait()
    loads[3].wait()
    for c in a_copies:
        c.wait_recv()

    lhs = unfold_halves(arecv[...].astype(F32)).reshape(nf * 8, width).astype(BF)
    which = lax.rem(lax.broadcasted_iota(jnp.int32, (nf * 8, 1), 0), 8) < 4
    hid = jnp.where(
        which,
        jnp.dot(lhs, win[0], preferred_element_type=F32),
        jnp.dot(lhs, win[1], preferred_element_type=F32),
    )
    hid = jax.nn.gelu(hid).astype(BF)
    out = jnp.where(
        which,
        jnp.dot(hid, wout[0], preferred_element_type=F32),
        jnp.dot(hid, wout[1], preferred_element_type=F32),
    )
    bsend[...] = out.reshape(nf, 8, width).astype(BF)
    every[t, f] = bsend[f]
    b_copies = []
    for d in range(1, nf):
        k = lax.rem(f + d, nf)
        c = remote(bsend.at[k], every.at[t, f], b_ss.at[d - 1], b_rs.at[d - 1], at_fc(k))
        c.start()
        b_copies.append(c)
    cross_combine(2)
    cross_combine(1)
    for c in b_copies:
        c.wait_recv()

    sides = ((h, t), (1 - h, x * 2 + 1 - h))
    pair_copies = []
    for n in range(NCH):
        ref = every.at[t, :, :, pl.ds(n * cw, cw)]
        c = remote(ref, ref, p_ss.at[n], p_rs.at[n], to_pair)
        c.start()
        pair_copies.append(c)
    g_copies = {}

    def send_out(b, n):
        if b == 1:
            pair_copies[n].wait_recv()
        ref = every.at[sides[b][1], :, :, pl.ds(n * cw, cw)]
        g_copies[b, n] = []
        for d in (1, 3, 2):
            c = remote(
                ref, ref, g_ss.at[b, n, d - 1], g_rs.at[b, n, d - 1], at_tok(lax.rem(x + d, 4) * 2 + h)
            )
            c.start()
            g_copies[b, n].append(c)

    state[13 * h] = jnp.zeros((128, width), BF)

    def mix(n):
        lane = pl.ds(n * cw, cw)
        for c in g_copies[0, n] + g_copies[1, n]:
            c.wait_recv()
        joined[n] = jnp.concatenate(
            [every[tt, ff, :, lane].astype(F32) for ff in range(nf) for tt in range(nt)], axis=0
        ).astype(BF)
        for base, count in ((0, 6), (6, 7)):
            rows = count * 128
            span = pl.ds(1 - h + base, count)
            mixed = jnp.dot(combine[span].reshape(rows, width), joined[n], preferred_element_type=F32)
            v = cells[span, :, lane].reshape(rows, cw).astype(F32) + mixed
            at = lax.broadcasted_iota(jnp.int32, (rows, 1), 0) + (8 * t - 2 - h + base) * 128
            inside = jnp.logical_and(at >= 0, at < 64 * 128)
            v = jnp.where(inside, v, 0.0)
            state[span, :, lane] = v.astype(BF).reshape(count, 128, cw)

    inner = jnp.where(h == 0, t > 0, t < nt - 1)

    def add_far_row(n):
        lane = pl.ds(n * cw, cw)
        mixed = jnp.dot(combine[13 * h], joined[n], preferred_element_type=F32)
        v = (cells[13 * h, :, lane].astype(F32) + mixed).astype(BF).astype(F32)
        v = jnp.where(inner, v, 0.0)
        for part in range(cw // 128):
            u = v[:, part * 128 : (part + 1) * 128]
            wide[part, pl.ds(8, 128), :] = u
            wide[part, pl.ds(0, 8), :] = u[120:128]
            wide[part, pl.ds(136, 8), :] = u[0:8]
            here = pl.ds(n * cw + part * 128, 128)
            terms = [wide[part, pl.ds(5 + b, 128), :] * cw_ref[6 * h, pl.ds(b, 1), here] for b in range(7)]
            conv[7 * h, :, here] = conv[7 * h, :, here] + tree_sum(terms)

    def convolve(k):
        lane = pl.ds(k * 128, 128)
        for tap in range(49):
            row = cw_ref[tap // 7, pl.ds(tap % 7, 1), lane]
            taps[tap] = jnp.broadcast_to(row, (16, 128)).astype(BF)

        @pl.loop(0, 14)
        def _(r):
            v = state[r, :, lane].astype(F32)
            wide[r, pl.ds(8, 128), :] = v
            wide[r, pl.ds(0, 8), :] = v[120:128]
            wide[r, pl.ds(136, 8), :] = v[0:8]

        @pl.loop(0, 8)
        def _(i):
            acc = [[None] * 4, [None] * 4]
            for b in range(7):
                wv = [taps[a * 7 + b] for a in range(7)]
                for blk in range(2):
                    start = i * 16 + (8 * blk + 5 + b)
                    v = [wide[r, pl.ds(start, 8), :] for r in range(14)]
                    pk = [jnp.concatenate([v[q], v[q + 4]], axis=0).astype(BF) for q in range(10)]
                    for p in range(4):
                        term = tree_sum(pk[p + a] * wv[a] for a in range(7))
                        acc[blk][p] = term if acc[blk][p] is None else acc[blk][p] + term
            for blk in range(2):
                for p in range(4):
                    val = acc[blk][p].astype(F32)
                    at = pl.multiple_of(i * 16 + 8 * blk, 8)
                    conv[p, pl.ds(at, 8), lane] = val[0:8]
                    conv[p + 4, pl.ds(at, 8), lane] = val[8:16]

    send_out(0, 0)
    send_out(0, 1)
    send_out(1, 0)
    send_out(1, 1)
    send_out(0, 2)
    send_out(1, 2)
    send_out(0, 3)
    send_out(1, 3)
    start_cross(LAST)
    mix(0)
    convolve(0)
    convolve(1)
    mix(1)
    convolve(2)
    convolve(3)
    mix(2)
    convolve(4)
    convolve(5)
    mix(3)
    convolve(6)
    convolve(7)
    cross_combine(0)
    for n in range(NCH):
        add_far_row(n)
    loads[4].wait()

    def norm_row(r, into):
        c = conv[r]
        center = c - jnp.mean(c, axis=-1, keepdims=True)
        spread = jnp.mean(center * center, axis=-1, keepdims=True)
        into[...] = (center * lax.rsqrt(spread + 1e-06) * lgain_ref[...]).astype(BF)

    def finish_row(r, source):
        branch = jnp.dot(source[...], proj[...], preferred_element_type=F32)
        res = state[r + 3].astype(F32) + scale_ref[...] * jax.nn.gelu(branch)
        outs[r] = res.astype(BF)
        pltpu.make_async_copy(outs.at[r], out_hbm.at[r], out_sem.at[r]).start()

    norm_row(0, even)

    @pl.loop(0, 4)
    def _(i):
        norm_row(2 * i + 1, odd)
        finish_row(2 * i, even)
        norm_row(jnp.minimum(2 * i + 2, 7), even)
        finish_row(2 * i + 1, odd)

    sent = peak_copies + y_copies + a_copies + b_copies + pair_copies + [top_copy]
    for group in (w_copies, x_copies, g_copies.values()):
        sent += [c for row in group for c in row]
    for c in sent:
        c.wait_send()

    @pl.when(t < nt - 1)
    def _():
        for p in range(3):
            halo_low(p).wait_send()

    @pl.when(t > 0)
    def _():
        for p in range(3):
            halo_high(p).wait_send()

    for r in range(8):
        pltpu.make_async_copy(outs.at[r], out_hbm.at[r], out_sem.at[r]).wait()


def fused(
    tokens, slot_keys, norm_gain, slot_gain, w_in, w_out, conv_weight, ln_gain, proj, layer_scale
):
    width = tokens.shape[2]
    vm = pl.BlockSpec(memory_space=pltpu.VMEM)
    anyspec = pl.BlockSpec(memory_space=pl.ANY)
    dma = pltpu.SemaphoreType.DMA
    nf = MEMBERS_AX
    return pl.pallas_call(
        mix_kernel,
        out_shape=jax.ShapeDtypeStruct((8, 128, width), BF),
        in_specs=[anyspec, anyspec, vm, vm, anyspec, anyspec, vm, vm, vm, anyspec],
        out_specs=anyspec,
        scratch_shapes=[
            pltpu.VMEM((14, 128, width), BF),
            pltpu.VMEM((width, width), BF),
            pltpu.VMEM(w_in.shape, BF),
            pltpu.VMEM(w_out.shape, BF),
            pltpu.VMEM((8, 128, width), F32),
            pltpu.VMEM((14, 128, width), BF),
            pltpu.VMEM((width, 1024), BF),
            pltpu.VMEM((nf, 4, 16, width), BF),
            pltpu.VMEM((2, 8, 16, width), BF),
            pltpu.VMEM((2, nf, 16, width), BF),
            pltpu.VMEM((nf * 8, width), BF),
            pltpu.VMEM((nf * 8, width), BF),
            pltpu.VMEM((nf * 8, width), F32),
            pltpu.VMEM((nf, 16, width // 2), BF),
            pltpu.VMEM((nf, 16, width // 2), BF),
            pltpu.VMEM((nf, 8, width), BF),
            pltpu.VMEM((8, nf, 8, width), BF),
            pltpu.VMEM((NCH, 1024, width // NCH), BF),
            pltpu.VMEM((14, 128, width), BF),
            pltpu.VMEM((14, 144, 128), F32),
            pltpu.VMEM((49, 16, 128), BF),
            pltpu.VMEM((8, 128, width), F32),
            pltpu.VMEM((128, width), BF),
            pltpu.VMEM((128, width), BF),
            pltpu.VMEM((8, 128, width), BF),
            pltpu.VMEM((width, width), BF),
            pltpu.VMEM((4, 1, width), F32),
            pltpu.VMEM((2, 1, width), F32),
            pltpu.VMEM((nf, 4, 16, 128), F32),
            dma((5,)),
            dma((3,)), dma((3,)),
            dma, dma,
            dma((2, 3)), dma((2, 3)),
            dma((NCH, 2)), dma((NCH, 2)),
            dma((NCH, 2)), dma((NCH, 2)),
            dma((NCH,)), dma((NCH,)),
            dma((15,)), dma((15,)),
            dma((15,)), dma((15,)),
            dma((NCH,)), dma((NCH,)),
            dma((2, NCH, 3)), dma((2, NCH, 3)),
            dma((8,)),
        ],
        compiler_params=pltpu.CompilerParams(
            collective_id=0, has_side_effects=True, vmem_limit_bytes=62 * 1024 * 1024
        ),
        name="fused",
    )(
        tokens, slot_keys, norm_gain.reshape(1, width), slot_gain.reshape(1, width), w_in, w_out,
        conv_weight, ln_gain.reshape(1, width), layer_scale.reshape(1, width), proj,
    )


def tree_sum(terms):
    terms = list(terms)
    while len(terms) > 1:
        nxt = [terms[i] + terms[i + 1] for i in range(0, len(terms) - 1, 2)]
        if len(terms) % 2:
            nxt.append(terms[-1])
        terms = nxt
    return terms[0]


def local(
    tokens, slot_keys, norm_gain, slot_gain, w_in, w_out, conv_weight, ln_gain, proj, layer_scale
):
    return fused(
        tokens[0], slot_keys, norm_gain, slot_gain, w_in, w_out, conv_weight, ln_gain, proj, layer_scale
    )[None]


def solution(mesh):
    in_specs = (
        P("fc", "tok", None, None),
        P(),
        P(),
        P(),
        P(("fc", "tok"), None, None),
        P(("fc", "tok"), None, None),
        P(),
        P(),
        P(),
        P(),
    )
    out_specs = P("fc", "tok", None, None)
    return jax.shard_map(local, mesh=mesh, in_specs=in_specs, out_specs=out_specs, check_vma=False)
```

```python
import jax
import jax.numpy as jnp
from jax import lax
from jax.experimental import pallas as pl
from jax.experimental.pallas import tpu as pltpu
from jax.sharding import PartitionSpec as P

BF = jnp.bfloat16
F32 = jnp.float32
MESH = pl.DeviceIdType.MESH
MEMBERS_AX = 16
NCH = 4
FIRST, EARLY, LAST = (2,), (1,), (0,)


def rms_scale(value, gain):
    return value * lax.rsqrt(jnp.mean(value * value, axis=-1, keepdims=True) + 1e-06) * gain


def fold_halves(v):
    half = v.shape[-1] // 2
    return jnp.concatenate([v[..., :half], v[..., half:]], axis=-2)


def unfold_halves(v):
    rows = v.shape[-2] // 2
    return jnp.concatenate([v[..., :rows, :], v[..., rows:, :]], axis=-1)


def mix_kernel(
    tok_hbm, keys_hbm, ngain_ref, sgain_ref, win_hbm, wout_hbm, cw_ref, lgain_ref, scale_ref, proj_hbm,
    out_hbm,
    cells, keys, win, wout, logits, combine, disp, numer, passed, rx, ysend, yrecv, keep,
    asend, arecv, bsend, every, joined, state, wide, taps, conv, even, odd, outs, proj, peaks, tops, shrink, load_sem,
    peak_ss, peak_rs, top_ss, top_rs, halo_ss, halo_rs, w_ss, w_rs, x_ss, x_rs, y_ss, y_rs, a_ss, a_rs, b_ss, b_rs,
    p_ss, p_rs, g_ss, g_rs, out_sem,
):
    nf, nt = MEMBERS_AX, 8
    width = cells.shape[2]
    cw = width // NCH
    f = lax.axis_index("fc")
    t = lax.axis_index("tok")
    x = lax.div(t, 2)
    h = lax.rem(t, 2)

    def at_tok(k):
        return {"fc": f, "tok": k}

    def at_fc(k):
        return {"fc": k, "tok": t}

    right, left, across = lax.rem(x + 1, 4), lax.rem(x + 3, 4), lax.rem(x + 2, 4)
    to_right, to_left, to_pair = at_tok(right * 2 + h), at_tok(left * 2 + h), at_tok(x * 2 + 1 - h)

    loads = [
        pltpu.make_async_copy(tok_hbm, cells.at[pl.ds(3, 8)], load_sem.at[0]),
        pltpu.make_async_copy(keys_hbm, keys, load_sem.at[1]),
        pltpu.make_async_copy(win_hbm, win, load_sem.at[2]),
        pltpu.make_async_copy(wout_hbm, wout, load_sem.at[3]),
        pltpu.make_async_copy(proj_hbm, proj, load_sem.at[4]),
    ]
    loads[0].start()
    loads[1].start()

    barrier = pltpu.get_barrier_semaphore()
    for d in range(1, nt):
        pl.semaphore_signal(barrier, inc=1, device_id=at_tok(lax.rem(t + d, nt)), device_id_type=MESH)
    for d in range(1, nf):
        pl.semaphore_signal(barrier, inc=1, device_id=at_fc(lax.rem(f + d, nf)), device_id_type=MESH)

    def remote(src, dst, ss, rs, dev):
        return pltpu.make_async_remote_copy(
            src_ref=src, dst_ref=dst, send_sem=ss, recv_sem=rs, device_id=dev, device_id_type=MESH
        )

    loads[0].wait()

    def halo_low(p):
        return remote(
            cells.at[8 + p], cells.at[p], halo_ss.at[0, p], halo_rs.at[0, p], at_tok(t + 1)
        )

    def halo_high(p):
        return remote(
            cells.at[3 + p], cells.at[11 + p], halo_ss.at[1, p], halo_rs.at[1, p], at_tok(t - 1)
        )

    def start_cross(parts):
        @pl.when(jnp.logical_and(h == 1, t < nt - 1))
        def _():
            for p in parts:
                halo_low(p).start()

        @pl.when(jnp.logical_and(h == 0, t > 0))
        def _():
            for p in parts:
                halo_high(2 - p).start()

    loads[1].wait()
    for c in loads[2:]:
        c.start()

    def logits_of(v):
        normed = rms_scale(v.astype(F32), ngain_ref[...]).astype(BF)
        return jnp.dot(normed, keys[...], preferred_element_type=F32)

    def softmax_of(l):
        e = jnp.exp(l - jnp.max(l, axis=-1, keepdims=True))
        return (e / jnp.sum(e, axis=-1, keepdims=True)).astype(BF)

    def first(r, peak):
        v = cells[pl.ds(3 + 2 * r, 2)].reshape(256, width)
        l = logits_of(v)
        logits[pl.ds(2 * r, 2)] = l.reshape(2, 128, width)
        return jnp.maximum(peak, jnp.max(l.reshape(32, 8, width), axis=0))

    def pure_combine():
        @pl.when(h == 1)
        def _():
            for p in range(3):
                halo_low(p).wait_recv()

        @pl.when(h == 0)
        def _():
            for p in range(3):
                halo_high(p).wait_recv()

        at = pl.ds(11 * (1 - h), 3)
        rows_in = cells[at].reshape(384, width)
        combine[at] = softmax_of(logits_of(rows_in)).reshape(3, 128, width)

    def cross_at(p):
        return p + h * (13 - 2 * p)

    def cross_combine(p):
        @pl.when(jnp.logical_and(h == 0, t > 0))
        def _():
            halo_low(p).wait_recv()

        @pl.when(jnp.logical_and(h == 1, t < nt - 1))
        def _():
            halo_high(2 - p).wait_recv()

        combine[cross_at(p)] = softmax_of(logits_of(cells[cross_at(p)]))

    peak = lax.fori_loop(0, 2, first, jnp.full((8, width), -jnp.inf, F32))
    pl.semaphore_wait(barrier, nt + nf - 2)

    start_cross(FIRST)
    peak = lax.fori_loop(2, 4, first, peak)
    mine = jnp.max(peak, axis=0, keepdims=True)
    peaks[x] = mine
    peak_copies = []
    for d in range(1, 4):
        k = lax.rem(x + d, 4)
        c = remote(peaks.at[x], peaks.at[x], peak_ss.at[d - 1], peak_rs.at[d - 1], at_tok(k * 2 + h))
        c.start()
        peak_copies.append(c)

    @pl.when(h == 0)
    def _():
        for p in range(3):
            halo_low(p).start()

    @pl.when(h == 1)
    def _():
        for p in range(3):
            halo_high(p).start()

    @pl.when(t == 0)
    def _():
        cells[pl.ds(0, 3)] = jnp.zeros((3, 128, width), BF)

    @pl.when(t == nt - 1)
    def _():
        cells[pl.ds(11, 3)] = jnp.zeros((3, 128, width), BF)


    @pl.loop(0, 8)
    def _(r):
        shifted = jnp.exp(logits[r] - mine)
        disp[:, pl.ds(pl.multiple_of(r * 128, 128), 128)] = shifted.T.astype(BF)

    @pl.loop(0, 8)
    def _(r):
        combine[3 + r] = softmax_of(logits[r])

    for c in peak_copies:
        c.wait_recv()
    top = jnp.maximum(jnp.maximum(peaks[0], peaks[1]), jnp.maximum(peaks[2], peaks[3]))
    tops[h] = top
    top_copy = remote(tops.at[h], tops.at[h], top_ss, top_rs, to_pair)
    top_copy.start()

    def as_column(row):
        return jnp.broadcast_to(row, (128, width)).T

    shrink[...] = as_column(jnp.exp(mine - top)).reshape(nf, 4, 16, 128)

    w_copies, x_copies = [], []

    def pass_on(n):
        lane = pl.ds(n * cw, cw)
        for c in w_copies[n]:
            c.wait_recv()
        numer[0:8, right, :, lane] = (
            numer[0:8, right, :, lane].astype(F32) + passed[0, :, :, lane].astype(F32)
        ).astype(BF)
        numer[8:16, left, :, lane] = (
            numer[8:16, left, :, lane].astype(F32) + passed[1, :, :, lane].astype(F32)
        ).astype(BF)
        row = [
            remote(numer.at[:, right, :, lane], rx.at[0, :, :, lane], x_ss.at[n, 0], x_rs.at[n, 0], to_right),
            remote(numer.at[:, left, :, lane], rx.at[1, :, :, lane], x_ss.at[n, 1], x_rs.at[n, 1], to_left),
        ]
        for c in row:
            c.start()
        x_copies.append(row)

    for n in range(NCH):
        lane = pl.ds(n * cw, cw)
        own = cells[pl.ds(3, 8), :, lane].reshape(1024, cw)
        factor = shrink[...].reshape(1024, 128)
        numer[:, :, :, lane] = (
            jnp.dot(disp[...], own, preferred_element_type=F32) * jnp.concatenate([factor] * (cw // 128), axis=1)
        ).astype(BF).reshape(nf, 4, 16, cw)
        low = pl.ds(0, 8)
        high = pl.ds(8, 8)
        row = [
            remote(
                numer.at[low, across, :, lane], passed.at[0, :, :, lane], w_ss.at[n, 0], w_rs.at[n, 0], to_right
            ),
            remote(
                numer.at[high, across, :, lane], passed.at[1, :, :, lane], w_ss.at[n, 1], w_rs.at[n, 1], to_left
            ),
        ]
        for c in row:
            c.start()
        w_copies.append(row)
        if n > 0:
            pass_on(n - 1)
    pass_on(NCH - 1)
    start_cross(EARLY)

    y_copies = []
    for n in range(NCH):
        lane = pl.ds(n * cw, cw)
        for c in x_copies[n]:
            c.wait_recv()
        total = numer[:, x, :, lane].astype(F32)
        for d in range(2):
            total = total + rx[d, :, :, lane].astype(F32)
        low = total[:, 0:8].reshape(nf * 8, cw)
        high = total[:, 8:16].reshape(nf * 8, cw)
        ysend[:, lane] = jnp.where(h == 0, high, low).astype(BF)
        keep[:, lane] = jnp.where(h == 0, low, high)
        c = remote(ysend.at[:, lane], yrecv.at[:, lane], y_ss.at[n], y_rs.at[n], to_pair)
        c.start()
        y_copies.append(c)

    top_copy.wait_recv()
    whole = jnp.maximum(tops[0], tops[1])

    def my_slots(row):
        shrink[...] = as_column(row).reshape(nf, 4, 16, 128)
        both = shrink[:, x]
        picked = jnp.where(h == 0, both[:, 0:8], both[:, 8:16]).reshape(nf * 8, 128)
        return jnp.concatenate([picked] * (width // 128), axis=1)

    keep[...] = keep[...] * my_slots(jnp.exp(tops[h] - whole))
    other = my_slots(jnp.exp(tops[1 - h] - whole))
    for c in y_copies:
        c.wait_recv()
    local_in = rms_scale(keep[...] + yrecv[...].astype(F32) * other, sgain_ref[...])
    asend[...] = fold_halves(local_in.reshape(nf, 8, width)).astype(BF)
    arecv[f] = asend[f]
    a_copies = []
    for d in range(1, nf):
        k = lax.rem(f + d, nf)
        c = remote(asend.at[k], arecv.at[f], a_ss.at[d - 1], a_rs.at[d - 1], at_fc(k))
        c.start()
        a_copies.append(c)
    pure_combine()
    loads[2].wait()
    loads[3].wait()
    for c in a_copies:
        c.wait_recv()

    lhs = unfold_halves(arecv[...].astype(F32)).reshape(nf * 8, width).astype(BF)
    which = lax.rem(lax.broadcasted_iota(jnp.int32, (nf * 8, 1), 0), 8) < 4
    hid = jnp.where(
        which,
        jnp.dot(lhs, win[0], preferred_element_type=F32),
        jnp.dot(lhs, win[1], preferred_element_type=F32),
    )
    hid = jax.nn.gelu(hid).astype(BF)
    out = jnp.where(
        which,
        jnp.dot(hid, wout[0], preferred_element_type=F32),
        jnp.dot(hid, wout[1], preferred_element_type=F32),
    )
    bsend[...] = out.reshape(nf, 8, width).astype(BF)
    every[t, f] = bsend[f]
    b_copies = []
    for d in range(1, nf):
        k = lax.rem(f + d, nf)
        c = remote(bsend.at[k], every.at[t, f], b_ss.at[d - 1], b_rs.at[d - 1], at_fc(k))
        c.start()
        b_copies.append(c)
    cross_combine(2)
    cross_combine(1)
    for c in b_copies:
        c.wait_recv()

    sides = ((h, t), (1 - h, x * 2 + 1 - h))
    pair_copies = []
    for n in range(NCH):
        ref = every.at[t, :, :, pl.ds(n * cw, cw)]
        c = remote(ref, ref, p_ss.at[n], p_rs.at[n], to_pair)
        c.start()
        pair_copies.append(c)
    g_copies = {}

    def send_out(b, n):
        if b == 1:
            pair_copies[n].wait_recv()
        ref = every.at[sides[b][1], :, :, pl.ds(n * cw, cw)]
        g_copies[b, n] = []
        for d in (1, 3, 2):
            c = remote(
                ref, ref, g_ss.at[b, n, d - 1], g_rs.at[b, n, d - 1], at_tok(lax.rem(x + d, 4) * 2 + h)
            )
            c.start()
            g_copies[b, n].append(c)

    state[13 * h] = jnp.zeros((128, width), BF)

    def mix(n):
        lane = pl.ds(n * cw, cw)
        for c in g_copies[0, n] + g_copies[1, n]:
            c.wait_recv()
        joined[n] = jnp.concatenate(
            [every[tt, ff, :, lane].astype(F32) for ff in range(nf) for tt in range(nt)], axis=0
        ).astype(BF)
        for base, count in ((0, 6), (6, 7)):
            rows = count * 128
            span = pl.ds(1 - h + base, count)
            mixed = jnp.dot(combine[span].reshape(rows, width), joined[n], preferred_element_type=F32)
            v = cells[span, :, lane].reshape(rows, cw).astype(F32) + mixed
            at = lax.broadcasted_iota(jnp.int32, (rows, 1), 0) + (8 * t - 2 - h + base) * 128
            inside = jnp.logical_and(at >= 0, at < 64 * 128)
            v = jnp.where(inside, v, 0.0)
            state[span, :, lane] = v.astype(BF).reshape(count, 128, cw)

    inner = jnp.where(h == 0, t > 0, t < nt - 1)

    def add_far_row(n):
        lane = pl.ds(n * cw, cw)
        mixed = jnp.dot(combine[13 * h], joined[n], preferred_element_type=F32)
        v = (cells[13 * h, :, lane].astype(F32) + mixed).astype(BF).astype(F32)
        v = jnp.where(inner, v, 0.0)
        for part in range(cw // 128):
            u = v[:, part * 128 : (part + 1) * 128]
            wide[part, pl.ds(8, 128), :] = u
            wide[part, pl.ds(0, 8), :] = u[120:128]
            wide[part, pl.ds(136, 8), :] = u[0:8]
            here = pl.ds(n * cw + part * 128, 128)
            terms = [wide[part, pl.ds(5 + b, 128), :] * cw_ref[6 * h, pl.ds(b, 1), here] for b in range(7)]
            conv[7 * h, :, here] = conv[7 * h, :, here] + tree_sum(terms)

    def convolve(k):
        lane = pl.ds(k * 128, 128)
        for tap in range(49):
            row = cw_ref[tap // 7, pl.ds(tap % 7, 1), lane]
            taps[tap] = jnp.broadcast_to(row, (16, 128)).astype(BF)

        @pl.loop(0, 14)
        def _(r):
            v = state[r, :, lane].astype(F32)
            wide[r, pl.ds(8, 128), :] = v
            wide[r, pl.ds(0, 8), :] = v[120:128]
            wide[r, pl.ds(136, 8), :] = v[0:8]

        @pl.loop(0, 8)
        def _(i):
            acc = [[None] * 4, [None] * 4]
            for b in range(7):
                wv = [taps[a * 7 + b] for a in range(7)]
                for blk in range(2):
                    start = i * 16 + (8 * blk + 5 + b)
                    v = [wide[r, pl.ds(start, 8), :] for r in range(14)]
                    pk = [jnp.concatenate([v[q], v[q + 4]], axis=0).astype(BF) for q in range(10)]
                    for p in range(4):
                        term = tree_sum(pk[p + a] * wv[a] for a in range(7))
                        acc[blk][p] = term if acc[blk][p] is None else acc[blk][p] + term
            for blk in range(2):
                for p in range(4):
                    val = acc[blk][p].astype(F32)
                    at = pl.multiple_of(i * 16 + 8 * blk, 8)
                    conv[p, pl.ds(at, 8), lane] = val[0:8]
                    conv[p + 4, pl.ds(at, 8), lane] = val[8:16]

    send_out(0, 0)
    send_out(0, 1)
    send_out(1, 0)
    send_out(1, 1)
    send_out(0, 2)
    send_out(1, 2)
    send_out(0, 3)
    send_out(1, 3)
    start_cross(LAST)
    mix(0)
    convolve(0)
    convolve(1)
    mix(1)
    convolve(2)
    convolve(3)
    mix(2)
    convolve(4)
    convolve(5)
    mix(3)
    convolve(6)
    convolve(7)
    cross_combine(0)
    for n in range(NCH):
        add_far_row(n)
    loads[4].wait()

    def norm_row(r, into):
        c = conv[r]
        center = c - jnp.mean(c, axis=-1, keepdims=True)
        spread = jnp.mean(center * center, axis=-1, keepdims=True)
        into[...] = (center * lax.rsqrt(spread + 1e-06) * lgain_ref[...]).astype(BF)

    def finish_row(r, source):
        branch = jnp.dot(source[...], proj[...], preferred_element_type=F32)
        res = state[r + 3].astype(F32) + scale_ref[...] * jax.nn.gelu(branch)
        outs[r] = res.astype(BF)
        pltpu.make_async_copy(outs.at[r], out_hbm.at[r], out_sem.at[r]).start()

    norm_row(0, even)

    @pl.loop(0, 4)
    def _(i):
        norm_row(2 * i + 1, odd)
        finish_row(2 * i, even)
        norm_row(jnp.minimum(2 * i + 2, 7), even)
        finish_row(2 * i + 1, odd)

    sent = peak_copies + y_copies + a_copies + b_copies + pair_copies + [top_copy]
    for group in (w_copies, x_copies, g_copies.values()):
        sent += [c for row in group for c in row]
    for c in sent:
        c.wait_send()

    @pl.when(t < nt - 1)
    def _():
        for p in range(3):
            halo_low(p).wait_send()

    @pl.when(t > 0)
    def _():
        for p in range(3):
            halo_high(p).wait_send()

    for r in range(8):
        pltpu.make_async_copy(outs.at[r], out_hbm.at[r], out_sem.at[r]).wait()


def fused(
    tokens, slot_keys, norm_gain, slot_gain, w_in, w_out, conv_weight, ln_gain, proj, layer_scale
):
    width = tokens.shape[2]
    vm = pl.BlockSpec(memory_space=pltpu.VMEM)
    anyspec = pl.BlockSpec(memory_space=pl.ANY)
    dma = pltpu.SemaphoreType.DMA
    nf = MEMBERS_AX
    return pl.pallas_call(
        mix_kernel,
        out_shape=jax.ShapeDtypeStruct((8, 128, width), BF),
        in_specs=[anyspec, anyspec, vm, vm, anyspec, anyspec, vm, vm, vm, anyspec],
        out_specs=anyspec,
        scratch_shapes=[
            pltpu.VMEM((14, 128, width), BF),
            pltpu.VMEM((width, width), BF),
            pltpu.VMEM(w_in.shape, BF),
            pltpu.VMEM(w_out.shape, BF),
            pltpu.VMEM((8, 128, width), F32),
            pltpu.VMEM((14, 128, width), BF),
            pltpu.VMEM((width, 1024), BF),
            pltpu.VMEM((nf, 4, 16, width), BF),
            pltpu.VMEM((2, 8, 16, width), BF),
            pltpu.VMEM((2, nf, 16, width), BF),
            pltpu.VMEM((nf * 8, width), BF),
            pltpu.VMEM((nf * 8, width), BF),
            pltpu.VMEM((nf * 8, width), F32),
            pltpu.VMEM((nf, 16, width // 2), BF),
            pltpu.VMEM((nf, 16, width // 2), BF),
            pltpu.VMEM((nf, 8, width), BF),
            pltpu.VMEM((8, nf, 8, width), BF),
            pltpu.VMEM((NCH, 1024, width // NCH), BF),
            pltpu.VMEM((14, 128, width), BF),
            pltpu.VMEM((14, 144, 128), F32),
            pltpu.VMEM((49, 16, 128), BF),
            pltpu.VMEM((8, 128, width), F32),
            pltpu.VMEM((128, width), BF),
            pltpu.VMEM((128, width), BF),
            pltpu.VMEM((8, 128, width), BF),
            pltpu.VMEM((width, width), BF),
            pltpu.VMEM((4, 1, width), F32),
            pltpu.VMEM((2, 1, width), F32),
            pltpu.VMEM((nf, 4, 16, 128), F32),
            dma((5,)),
            dma((3,)), dma((3,)),
            dma, dma,
            dma((2, 3)), dma((2, 3)),
            dma((NCH, 2)), dma((NCH, 2)),
            dma((NCH, 2)), dma((NCH, 2)),
            dma((NCH,)), dma((NCH,)),
            dma((15,)), dma((15,)),
            dma((15,)), dma((15,)),
            dma((NCH,)), dma((NCH,)),
            dma((2, NCH, 3)), dma((2, NCH, 3)),
            dma((8,)),
        ],
        compiler_params=pltpu.CompilerParams(
            collective_id=0, has_side_effects=True, vmem_limit_bytes=62 * 1024 * 1024
        ),
        name="fused",
    )(
        tokens, slot_keys, norm_gain.reshape(1, width), slot_gain.reshape(1, width), w_in, w_out,
        conv_weight, ln_gain.reshape(1, width), layer_scale.reshape(1, width), proj,
    )


def tree_sum(terms):
    terms = list(terms)
    while len(terms) > 1:
        nxt = [terms[i] + terms[i + 1] for i in range(0, len(terms) - 1, 2)]
        if len(terms) % 2:
            nxt.append(terms[-1])
        terms = nxt
    return terms[0]


def local(
    tokens, slot_keys, norm_gain, slot_gain, w_in, w_out, conv_weight, ln_gain, proj, layer_scale
):
    return fused(
        tokens[0], slot_keys, norm_gain, slot_gain, w_in, w_out, conv_weight, ln_gain, proj, layer_scale
    )[None]


def solution(mesh):
    in_specs = (
        P("fc", "tok", None, None),
        P(),
        P(),
        P(),
        P(("fc", "tok"), None, None),
        P(("fc", "tok"), None, None),
        P(),
        P(),
        P(),
        P(),
    )
    out_specs = P("fc", "tok", None, None)
    return jax.shard_map(local, mesh=mesh, in_specs=in_specs, out_specs=out_specs, check_vma=False)
```
